32 devices in a mesh: node: 8 (over y, x, core), grp: 4 (over z).
Axes of the slice: x: 2, y: 2, z: 4, core: 2. Of those that a mesh axis runs over, the one named last changes fastest.
Arguments:
- tokens: bfloat16 [12288, 1792], P(('node', 'grp')), may hold values from -6 to 6
- cotangent: bfloat16 [12288, 1792], P(('node', 'grp')), may hold values from -6 to 6
- gate_weight: bfloat16 [1792, 1024], P('node'), may hold values from -0.125 to 0.125
- up_weight: bfloat16 [1792, 1024], P('node'), may hold values from -0.125 to 0.125
- down_weight_t: bfloat16 [1792, 1024], P('node'), may hold values from -0.125 to 0.125
- error_memory: bfloat16 [4, 1792, 3072], P('grp', 'node'), may hold values from -4 to 4
- q_init: float32 [3, 1024, 32], replicated, may hold values from -6 to 6
Outputs:
- token_grad: bfloat16 [12288, 1792], P(('node', 'grp'))
- new_error: bfloat16 [4, 1792, 3072], P('grp', 'node')
- p_hat: float32 [3, 1792, 32], P(None, 'node')
- q_new: float32 [3, 1024, 32], replicated
The draws below stay inside these ranges and needn't reach their ends.
All inputs are finite; a program needn't handle non-finite values.
Results may differ from the reference program's by a relative error of at most 0.012.
Values may be sent and summed in bfloat16 or wider, within the bound.
A program may use at most 192 MiB of HBM per device.

```python
import math
import jax
import jax.numpy as jnp
from jax import lax

D = 1792
H = 1024
R = 32
TOK_DEV = 384
TOKENS = 12288
N_NODE = 8
N_GRP = 4


def block_levels(rng, dims, cuts, least, high):
    factor_of, own = 1.0, jax.random.fold_in(rng, 6)
    for position, parts in cuts:
        heights = jnp.exp(jax.random.uniform(jax.random.fold_in(own, position), (parts,), jnp.float32, least / len(cuts), high / len(cuts)))
        factor_of = factor_of * jnp.repeat(heights, dims[position] // parts).reshape([-1 if axis == position else 1 for axis in range(len(dims))])
    return factor_of


def normal_values(own_key, extent, scale, bound, pieces=(), kind=jnp.bfloat16):
    entries = jax.random.normal(own_key, extent, jnp.float32) * scale
    if len(pieces) > 0:
        entries = block_levels(own_key, extent, pieces, -0.22, 0.18) * entries
    return jnp.clip(entries, min=-bound, max=bound).astype(kind)


def setup_inputs(seed: int = 0) -> dict:
    arg_keys = jax.random.split(jax.random.key(seed), 8)
    return {
        "tokens": normal_values(arg_keys[0], (TOKENS, D), 1.0, 6.0, ((0, 32),)),
        "cotangent": normal_values(arg_keys[1], (TOKENS, D), 1.0, 6.0, ((0, 32),)),
        "gate_weight": normal_values(arg_keys[2], (D, H), D ** -0.5, 0.125, ((0, 8),)),
        "up_weight": normal_values(arg_keys[3], (D, H), D ** -0.5, 0.125, ((0, 8),)),
        "down_weight_t": normal_values(arg_keys[4], (D, H), D ** -0.5, 0.125, ((0, 8),)),
        "error_memory": normal_values(arg_keys[5], (N_GRP, D, 3 * H), 0.5, 4.0, ((0, 4), (1, 8))),
        "q_init": normal_values(arg_keys[6], (3, H, R), 1.0, 6.0, (), jnp.float32),
    }


def gelu_parts(value):
    coeff = math.sqrt(2.0 / math.pi)
    inner = coeff * (value + 0.044715 * value * value * value)
    tanh_value = jnp.tanh(inner)
    activation = 0.5 * value * (1.0 + tanh_value)
    slope = 0.5 * (1.0 + tanh_value) + 0.5 * value * (1.0 - tanh_value * tanh_value) * coeff * (1.0 + 3.0 * 0.044715 * value * value)
    return (activation, slope)

def arrange(values):
    return values.reshape(N_NODE, N_GRP, TOK_DEV, -1).transpose(1, 0, 2, 3).reshape(N_GRP, N_NODE * TOK_DEV, -1)

def group_grad(items):
    token_rows, cot_rows, gate_up, hidden = items
    left_part = jnp.dot(token_rows.T.astype(jnp.float32), gate_up.astype(jnp.float32), preferred_element_type=jnp.float32)
    right_part = jnp.dot(cot_rows.T.astype(jnp.float32), hidden.astype(jnp.float32), preferred_element_type=jnp.float32)
    return jnp.concatenate([left_part, right_part], axis=1)

def reference(tokens, cotangent, gate_weight, up_weight, down_weight_t, error_memory, q_init):
    hidden_units = gate_weight.shape[1]
    gate_pre = jnp.dot(tokens.astype(jnp.float32), gate_weight.astype(jnp.float32), preferred_element_type=jnp.float32)
    up_pre = jnp.dot(tokens.astype(jnp.float32), up_weight.astype(jnp.float32), preferred_element_type=jnp.float32)
    activation, slope = gelu_parts(gate_pre)
    hidden = (activation * up_pre).astype(jnp.bfloat16)
    back_hidden = jnp.dot(cotangent.astype(jnp.float32), down_weight_t.astype(jnp.float32), preferred_element_type=jnp.float32)
    grad_up = (back_hidden * activation).astype(jnp.bfloat16)
    grad_gate = (back_hidden * up_pre * slope).astype(jnp.bfloat16)
    token_grad = (jnp.dot(grad_gate.astype(jnp.float32), gate_weight.T.astype(jnp.float32), preferred_element_type=jnp.float32) + jnp.dot(grad_up.astype(jnp.float32), up_weight.T.astype(jnp.float32), preferred_element_type=jnp.float32)).astype(jnp.bfloat16)
    gate_up = jnp.concatenate([grad_gate, grad_up], axis=1)
    grads = lax.map(group_grad, (arrange(tokens), arrange(cotangent), arrange(gate_up), arrange(hidden)))
    grad_scale = 1.0 / math.sqrt(TOK_DEV * N_NODE)
    merged = grads * grad_scale + error_memory.astype(jnp.float32)
    hats = []
    rights = []
    errors = []
    for m in range(3):
        matrix_block = merged[:, :, m * hidden_units:(m + 1) * hidden_units]
        power = jnp.einsum('kdh,hr->dr', matrix_block, q_init[m], precision=lax.Precision.HIGHEST) / N_GRP
        gram_matrix = jnp.dot(power.T, power, precision=lax.Precision.HIGHEST)
        factor = jnp.linalg.cholesky(gram_matrix)
        left_hat = jax.scipy.linalg.solve_triangular(factor, power.T, lower=True).T
        right_new = jnp.einsum('kdh,dr->hr', matrix_block, left_hat, precision=lax.Precision.HIGHEST) / N_GRP
        rebuilt = jnp.dot(left_hat, right_new.T, precision=lax.Precision.HIGHEST)
        errors.append(matrix_block - rebuilt[None])
        hats.append(left_hat)
        rights.append(right_new)
    new_error = jnp.concatenate(errors, axis=2).astype(jnp.bfloat16)
    return (token_grad, new_error, jnp.stack(hats), jnp.stack(rights))
```

```python
import functools
import math

import jax
import jax.numpy as jnp
from jax import lax
from jax.experimental import pallas as pl
from jax.experimental.pallas import tpu as pltpu
from jax.sharding import PartitionSpec as P

MESH = pl.DeviceIdType.MESH
F32, BF16 = jnp.float32, jnp.bfloat16
HIGHEST = lax.Precision.HIGHEST
LANES = 128


def gelu_parts(value):
    coeff = math.sqrt(2.0 / math.pi)
    square = value * value
    tanh_value = jnp.tanh(coeff * (value + 0.044715 * square * value))
    activation = 0.5 * value * (1.0 + tanh_value)
    slope = 0.5 * (1.0 + tanh_value) + 0.5 * value * (1.0 - tanh_value * tanh_value) * coeff * (
        1.0 + 3.0 * 0.044715 * square
    )
    return activation, slope


def dot(a, b, precision=None):
    return jnp.dot(a, b, preferred_element_type=F32, precision=precision)


def dot_nt(a, b, precision=None):
    return lax.dot_general(
        a, b, (((1,), (1,)), ((), ())), preferred_element_type=F32, precision=precision
    )


def subsets(items):
    found = [()]
    for item in items:
        found += [s + (item,) for s in found]
    return found


def kernel(
    n, g, rank,
    tok_hbm, cot_hbm, w_gate, w_up, w_down, err_hbm, q_hbm,
    tok_grad, new_err, p_out, q_out,
    full, tok, cot, turned, turned_in, acts, ups, mine, theirs, grads, *rest
):
    bits = n.bit_length() - 1
    recv_bufs = rest[:bits - 1]
    (high, low, q_right, err, q_rows, tok_out, err_out, pw_acc, power, block_diag, q_t, pw_all,
     gram_all, q_part, q_rs, q_grp, q_all, send_sems, recv_sems, local_sems) = rest[bits - 1:]
    me, grp = lax.axis_index("node"), lax.axis_index("grp")
    rows, hidden = w_gate.shape
    tokens, depth = tok.shape
    side = depth // 2
    wide = 2 * LANES
    chunks = hidden // wide
    used = 3 * rank
    weights = (w_gate, w_up, w_down)

    barrier = pltpu.get_barrier_semaphore()
    for d in range(1, n):
        pl.semaphore_signal(barrier, inc=1, device_id=(lax.rem(me + d, n), grp), device_id_type=MESH)
    for d in range(1, g):
        pl.semaphore_signal(barrier, inc=1, device_id=(me, lax.rem(grp + d, g)), device_id_type=MESH)

    flip = [(1 << b) * (1 - 2 * lax.rem(me // (1 << b), 2)) for b in range(bits)]
    offset = lambda mask: sum((flip[b] for b in mask), 0)
    pair = me + flip[0]
    core = lax.rem(me, 2)
    half_node = me // 2
    half_flip = [0] + [
        (1 << (b - 1)) * (1 - 2 * lax.rem(me // (1 << b), 2)) for b in range(1, bits)
    ]
    half_offset = lambda mask: sum((half_flip[b] for b in mask), 0)
    plane = lax.rem(grp, 2)
    twin = grp + 1 - 2 * plane
    outer = list(range(1, bits))
    orders = [outer, outer[::-1]]
    steps = len(outer)
    block = lambda index: pl.ds(pl.multiple_of(index * rows, rows), rows)

    locals_count = [0]

    def local(src, dst):
        copy = pltpu.make_async_copy(src, dst, local_sems.at[locals_count[0]])
        locals_count[0] += 1
        copy.start()
        return copy

    loads = []
    for c in range(chunks):
        loads.append([
            local(weights[w].at[:, pl.ds(j * LANES, LANES)], full.at[j, w, block(me)])
            for j in (2 * c, 2 * c + 1) for w in range(3)
        ])
    cot_load = local(cot_hbm, cot)
    tok_load = local(tok_hbm, tok)
    q_load = local(q_hbm, q_rows.at[0:used])
    err_load = local(err_hbm.at[0], err)

    count = [0]
    started = []

    def send(src, dst, node, group):
        copy = pltpu.make_async_remote_copy(
            src_ref=src, dst_ref=dst,
            send_sem=send_sems.at[count[0]], recv_sem=recv_sems.at[count[0]],
            device_id=(node, group), device_id_type=MESH,
        )
        count[0] += 1
        started.append(copy)
        copy.start()
        return copy

    if rows % 32 == 0:
        parts = [[(0, rows // 2, 0), (rows // 2, rows // 2, 1)]] * chunks
    else:
        parts = [[(0, rows, c % 2)] for c in range(chunks)]

    def piece(j, mask, part):
        start = (me + offset(mask)) * rows + part[0]
        return full.at[j, :, pl.ds(pl.multiple_of(start, math.gcd(rows, part[1])), part[1]), :]

    arrivals, across, inside = {}, {}, {}

    def gather_send(c, t, part):
        order = orders[part[2]]
        for mask in subsets(order[:t]):
            at = piece(2 * c + plane, mask, part)
            copy = send(at, at, me + flip[order[t]], grp)
            arrivals.setdefault((c, t, part), []).append((copy, mask + (order[t],)))

    def gather_step(c, t):
        for part in parts[c]:
            for copy, _ in arrivals[c, t, part]:
                copy.wait_recv()
            if t + 1 < steps:
                gather_send(c, t + 1, part)
            for _, mask in arrivals[c, t, part]:
                at = piece(2 * c + plane, mask, part)
                across.setdefault(c, []).append((send(at, at, me, twin), mask, part))
                inside.setdefault(c, []).append(send(at, at, pair, grp))

    def gather_finish(c):
        for copy, mask, part in across[c]:
            copy.wait_recv()
            at = piece(2 * c + 1 - plane, mask, part)
            inside[c].append(send(at, at, pair, grp))
        for copy in inside[c]:
            copy.wait_recv()

    pl.semaphore_wait(barrier, n - 1 + g - 1)

    def launch(c):
        for copy in loads[c]:
            copy.wait()
        for part in parts[c]:
            gather_send(c, 0, part)
        at = full.at[pl.ds(2 * c, 2), :, block(me), :]
        inside.setdefault(c, []).append(send(at, at, pair, grp))

    for c in range(min(2, chunks)):
        launch(c)

    pw_acc[...] = jnp.zeros_like(pw_acc)
    power[...] = jnp.zeros_like(power)
    block_diag[...] = jnp.zeros_like(block_diag)
    q_t[...] = jnp.zeros_like(q_t)
    for buf in (high, low):
        for m in range(3):
            buf[m, rows:, :] = jnp.zeros((buf.shape[1] - rows, hidden), BF16)

    def turn(which, i):
        src = (tok, cot)[which]
        tile = src[:, i * wide:(i + 1) * wide].T
        first = i * wide
        while first < (i + 1) * wide:
            b = first // rows
            last = min((b + 1) * rows, (i + 1) * wide)
            at = (b // 2) * rows + first - b * rows
            turned[which, b % 2, at:at + last - first, :] = tile[first - i * wide:last - i * wide]
            first = last

    def right_factors():
        q_load.wait()
        q_rows[used:, :] = jnp.zeros((LANES - used, hidden), F32)
        lane = lax.broadcasted_iota(jnp.int32, (wide, LANES), 1)
        for c in range(chunks):
            at = slice(c * wide, (c + 1) * wide)
            columns = q_rows[:, at].T
            top = columns.astype(BF16)
            bottom = (columns - top.astype(F32)).astype(BF16)
            for m in range(3):
                inside_m = (lane >= m * rank) & (lane < (m + 1) * rank)
                q_right[m, at, 0:LANES] = jnp.where(inside_m, top.astype(F32), 0.0).astype(BF16)
                q_right[m, at, LANES:] = jnp.where(inside_m, bottom.astype(F32), 0.0).astype(BF16)

    filler = []
    for which, load in ((1, cot_load), (0, tok_load)):
        filler.append(load.wait)
        for i in range(depth // wide):
            filler.append(functools.partial(turn, which, i))
        filler.append(lambda which=which: turned_sends.append(
            send(turned.at[which, 1 - core], turned_in.at[which], pair, grp)))
    filler.append(right_factors)
    turned_sends = []

    events = sorted(
        ((c, t) for c in range(chunks) for t in range(steps)), key=lambda e: (2 * e[1] + e[0], -e[1])
    )
    each = -(-len(filler) // len(events))
    for c, t in events:
        for work in filler[:each]:
            work()
        filler = filler[each:]
        gather_step(c, t)
        if t == 0 and c + 2 < chunks:
            launch(c + 2)
    for work in filler:
        work()

    def columns_of(c, w):
        return jnp.concatenate([full[2 * c, w], full[2 * c + 1, w]], axis=1)

    def forward(c):
        acts[...] = dot(tok[...], columns_of(c, 0))
        up_pre = dot(tok[...], columns_of(c, 1))
        activation, slope = gelu_parts(acts[...])
        acts[...] = activation
        ups[...] = up_pre * slope
        mine[c, 0] = (activation * up_pre).astype(BF16)

    def backward(c):
        back = dot(cot[...], columns_of(c, 2))
        mine[c, 1] = (back * ups[...]).astype(BF16)
        mine[c, 2] = (back * acts[...]).astype(BF16)

    tile = side // 2

    def gradient(c, m):
        which, k = (1, 0) if m == 2 else (0, m + 1)
        right = jnp.concatenate([mine[c, k], theirs[c, k]], axis=0)
        for i in range(2):
            at = pl.ds(i * tile, tile)
            left = jnp.concatenate([turned[which, core, at, :], turned_in[which, at, :]], axis=1)
            part = dot(left, right).astype(BF16)
            grads[c, m, 0, at, :] = part[:, 0:LANES]
            grads[c, m, 1, at, :] = part[:, LANES:]

    reduces = {}

    def reduce_start(c, m, t):
        for h in range(2):
            bit = orders[h][t]
            reduces[c, m, t, h] = []
            for slot, mask in enumerate(subsets(orders[h][t + 1:])):
                src = grads.at[c, m, h, block(half_node + half_flip[bit] + half_offset(mask))]
                dst = recv_bufs[t].at[(c * 3 + m) * 2 + h, slot]
                reduces[c, m, t, h].append(send(src, dst, me + flip[bit], grp))

    scale = 1.0 / math.sqrt(tokens * n)

    def reduce_add(c, m, t):
        for h in range(2):
            for slot, mask in enumerate(subsets(orders[h][t + 1:])):
                reduces[c, m, t, h][slot].wait_recv()
                at = block(half_node + half_offset(mask))
                total = (
                    grads[c, m, h, at, :].astype(F32)
                    + recv_bufs[t][(c * 3 + m) * 2 + h, slot].astype(F32)
                )
                if t < steps - 1:
                    grads[c, m, h, at, :] = total.astype(BF16)
                else:
                    first = c * wide + h * LANES
                    memory = err[:, m * hidden + first:m * hidden + first + LANES].astype(F32)
                    merged = total * scale + memory
                    top = merged.astype(BF16)
                    high[m, 0:rows, first:first + LANES] = top
                    low[m, 0:rows, first:first + LANES] = (merged - top.astype(F32)).astype(BF16)

    def advance(c, m, t):
        reduce_add(c, m, t - 1)
        reduce_start(c, m, t)

    def reduce_finish(c, m):
        reduce_add(c, m, steps - 1)
        at = slice(c * wide, (c + 1) * wide)
        both = dot(high[m, 0:rows, at], q_right[m, at, :])
        rest_part = dot(low[m, 0:rows, at], q_right[m, at, 0:LANES])
        pw_acc[...] += both[:, 0:LANES] + both[:, LANES:] + rest_part

    def token_part(i):
        at = slice(i * wide, (i + 1) * wide)
        total = jnp.zeros((tokens, wide), F32)
        for k in (1, 2):
            left = jnp.concatenate([mine[c, k] for c in range(chunks)], axis=1)
            right = jnp.concatenate([full[j, k - 1, at, :] for j in range(2 * chunks)], axis=1)
            total += dot_nt(left, right)
        tok_out[:, at] = total.astype(BF16)
        token_writes.append(local(tok_out.at[:, at], tok_grad.at[:, at]))

    token_writes = []
    token_tiles = list(range(depth // wide))

    def token_work(amount):
        for _ in range(min(amount, len(token_tiles))):
            token_part(token_tiles.pop(0))

    order_m = (2, 0, 1)
    for c in range(chunks):
        gather_finish(c)
        forward(c)
        hid_copy = send(mine.at[c, 0], theirs.at[c, 0], pair, grp)
        backward(c)
        back_copy = send(mine.at[c, pl.ds(1, 2)], theirs.at[c, pl.ds(1, 2)], pair, grp)
        if c == 0:
            err_load.wait()
            for copy in turned_sends:
                copy.wait_recv()
        hid_copy.wait_recv()
        gradient(c, 2)
        reduce_start(c, 2, 0)
        back_copy.wait_recv()
        for m in (0, 1):
            gradient(c, m)
            reduce_start(c, m, 0)
        if c > 0:
            for m in order_m:
                reduce_finish(c - 1, m)
        if c == chunks - 1:
            token_work(3)
        for t in range(1, steps):
            for m in order_m:
                advance(c, m, t)
                if c == chunks - 1:
                    token_work(2)
    token_work(len(token_tiles))
    for m in order_m:
        reduce_finish(chunks - 1, m)

    pw_all[grp] = pw_acc[...].astype(BF16)
    copies = [
        send(pw_all.at[grp], pw_all.at[grp], me, lax.rem(grp + d, g)) for d in range(1, g)
    ]
    for copy in copies:
        copy.wait_recv()
    total = pw_all[0].astype(F32)
    for k in range(1, g):
        total += pw_all[k].astype(F32)
    power[0:rows, :] = total * (1.0 / g)

    lane = lax.broadcasted_iota(jnp.int32, (rank, LANES), 1)
    row = lax.broadcasted_iota(jnp.int32, (rank, LANES), 0)
    padded = power[...]
    gram = dot(padded.T, padded, HIGHEST)
    picked = gram[0:rank]
    for m in range(1, 3):
        picked = jnp.where(lane >= m * rank, gram[m * rank:(m + 1) * rank], picked)
    gram_all[me] = picked
    copies = [
        send(gram_all.at[me], gram_all.at[me], lax.rem(me + d, n), grp) for d in range(1, n)
    ]
    for copy in copies:
        copy.wait_recv()
    picked = gram_all[0]
    for k in range(1, n):
        picked += gram_all[k]

    work = []
    for m in range(3):
        rolled = picked if m == 0 else pltpu.roll(picked, LANES - m * rank, 1)
        unit = jnp.where(lane == row + rank, 1.0, 0.0).astype(F32)
        work.append(jnp.where(lane < rank, rolled, unit))
    for j in range(rank):
        for m in range(3):
            a = work[m]
            inverse = 1.0 / jnp.sqrt(a[j:j + 1, j:j + 1])
            pivot_row = a[j:j + 1, :] * inverse
            column = a[:, j:j + 1] * inverse
            work[m] = jnp.where(row > j, a - column * pivot_row, jnp.where(row == j, pivot_row, a))
    for m in range(3):
        shift = ((m - 1) * rank) % LANES
        moved = work[m] if shift == 0 else pltpu.roll(work[m], shift, 1)
        inside_m = (lane >= m * rank) & (lane < (m + 1) * rank)
        block_diag[m * rank:(m + 1) * rank, :] = jnp.where(inside_m, moved, 0.0)
    hat_t = dot_nt(block_diag[...], power[...], HIGHEST)
    hat = dot_nt(power[0:rows, :], block_diag[...], HIGHEST)
    p_out[...] = hat_t[0:used, 0:rows]

    c_blocks = min(n, hidden // LANES)
    r_blocks = n // c_blocks
    c_size, r_size = hidden // c_blocks, used // r_blocks
    hat_top = hat_t.astype(BF16)
    hat_bottom = (hat_t - hat_top.astype(F32)).astype(BF16)
    for m in range(3):
        at = slice(m * rank, (m + 1) * rank)
        left = jnp.concatenate([hat_top[at], hat_bottom[at]], axis=0)
        both = dot(left, high[m])
        q_t[at, :] = both[0:rank] + both[rank:]
    spots = [
        (slice(c // c_blocks * r_size, (c // c_blocks + 1) * r_size),
         slice(c % c_blocks * c_size, (c % c_blocks + 1) * c_size))
        for c in range(n)
    ]
    for c in range(n):
        q_part[c] = q_t[spots[c]].astype(BF16)
    q_rs[me] = q_part[me]
    copies = []
    for d in range(1, n):
        to = lax.rem(me + d, n)
        copies.append(send(q_part.at[to], q_rs.at[me], to, grp))
    for copy in copies:
        copy.wait_recv()
    total = q_rs[0].astype(F32)
    for k in range(1, n):
        total += q_rs[k].astype(F32)
    q_grp[grp] = total.astype(BF16)
    copies = [send(q_grp.at[grp], q_grp.at[grp], me, lax.rem(grp + d, g)) for d in range(1, g)]
    for copy in copies:
        copy.wait_recv()
    total = q_grp[0].astype(F32)
    for k in range(1, g):
        total += q_grp[k].astype(F32)
    q_all[me] = (total * (1.0 / g)).astype(BF16)
    copies = [send(q_all.at[me], q_all.at[me], lax.rem(me + d, n), grp) for d in range(1, n)]
    for copy in copies:
        copy.wait_recv()
    for c in range(n):
        q_t[spots[c]] = q_all[c].astype(F32)
    q_out[...] = q_t[0:used, :]

    lanes = lax.broadcasted_iota(jnp.int32, (rows, LANES), 1)
    right = q_t[...].astype(BF16)
    right = jnp.concatenate([right, right], axis=0)
    writes = []
    for m in range(3):
        own = jnp.where((lanes >= m * rank) & (lanes < (m + 1) * rank), hat, 0.0)
        top = own.astype(BF16)
        left = jnp.concatenate([top, (own - top.astype(F32)).astype(BF16)], axis=1)
        for c in range(chunks):
            at = slice(c * wide, (c + 1) * wide)
            rebuilt = dot(left, right[:, at])
            merged = high[m, 0:rows, at].astype(F32) + low[m, 0:rows, at].astype(F32)
            err_out[:, m * hidden + c * wide:m * hidden + (c + 1) * wide] = (
                merged - rebuilt
            ).astype(BF16)
        at = pl.ds(m * hidden, hidden)
        writes.append(local(err_out.at[:, at], new_err.at[0, :, at]))
    for copy in started:
        copy.wait_send()
    for copy in token_writes + writes:
        copy.wait()


def on_device(n, g, tokens, cotangent, gate_weight, up_weight, down_weight_t, error_memory, q_init):
    token_rows, depth = tokens.shape
    rows, hidden = gate_weight.shape
    rank = q_init.shape[2]
    used = 3 * rank
    bits = n.bit_length() - 1
    side = depth // 2
    wide = 2 * LANES
    chunks = hidden // wide
    padded = -(-rows // LANES) * LANES
    q_rows = q_init.transpose(0, 2, 1).reshape(used, hidden)
    c_blocks = min(n, hidden // LANES)
    chunk = (used // (n // c_blocks), hidden // c_blocks)
    others = n // 2 - 1
    parts = 2 if rows % 32 == 0 else 1
    copies = (
        chunks * (1 + parts * 4 * others) + chunks * 6 * others + 2 * chunks + 2
        + 3 * (n - 1) + 2 * (g - 1)
    )
    copies_here = 6 * chunks + 4 + depth // wide + 3
    recv_shapes = [
        pltpu.VMEM((chunks * 6, 1 << (bits - 2 - t), rows, LANES), BF16) for t in range(bits - 1)
    ]
    vmem = pl.BlockSpec(memory_space=pltpu.VMEM)
    hbm = pl.BlockSpec(memory_space=pl.ANY)
    token_grad, new_error, hat_t, q_t = pl.pallas_call(
        functools.partial(kernel, n, g, rank),
        out_shape=(
            jax.ShapeDtypeStruct((token_rows, depth), BF16),
            jax.ShapeDtypeStruct((1, rows, 3 * hidden), BF16),
            jax.ShapeDtypeStruct((used, rows), F32),
            jax.ShapeDtypeStruct((used, hidden), F32),
        ),
        in_specs=[hbm] * 7,
        out_specs=(hbm, hbm, vmem, vmem),
        scratch_shapes=[
            pltpu.VMEM((2 * chunks, 3, depth, LANES), BF16),
            pltpu.VMEM((token_rows, depth), BF16),
            pltpu.VMEM((token_rows, depth), BF16),
            pltpu.VMEM((2, 2, side, token_rows), BF16),
            pltpu.VMEM((2, side, token_rows), BF16),
            pltpu.VMEM((token_rows, wide), F32),
            pltpu.VMEM((token_rows, wide), F32),
            pltpu.VMEM((chunks, 3, token_rows, wide), BF16),
            pltpu.VMEM((chunks, 3, token_rows, wide), BF16),
            pltpu.VMEM((chunks, 3, 2, side, LANES), BF16),
            *recv_shapes,
            pltpu.VMEM((3, padded, hidden), BF16),
            pltpu.VMEM((3, padded, hidden), BF16),
            pltpu.VMEM((3, hidden, wide), BF16),
            pltpu.VMEM((rows, 3 * hidden), BF16),
            pltpu.VMEM((LANES, hidden), F32),
            pltpu.VMEM((token_rows, depth), BF16),
            pltpu.VMEM((rows, 3 * hidden), BF16),
            pltpu.VMEM((rows, LANES), F32),
            pltpu.VMEM((padded, LANES), F32),
            pltpu.VMEM((LANES, LANES), F32),
            pltpu.VMEM((LANES, hidden), F32),
            pltpu.VMEM((g, rows, LANES), BF16),
            pltpu.VMEM((n, rank, LANES), F32),
            pltpu.VMEM((n,) + chunk, BF16),
            pltpu.VMEM((n,) + chunk, BF16),
            pltpu.VMEM((g,) + chunk, BF16),
            pltpu.VMEM((n,) + chunk, BF16),
            pltpu.SemaphoreType.DMA((copies,)),
            pltpu.SemaphoreType.DMA((copies,)),
            pltpu.SemaphoreType.DMA((copies_here,)),
        ],
        compiler_params=pltpu.CompilerParams(
            collective_id=0, has_side_effects=True, vmem_limit_bytes=67_043_328
        ),
    )(tokens, cotangent, gate_weight, up_weight, down_weight_t, error_memory, q_rows)
    p_hat = hat_t.reshape(3, rank, rows).transpose(0, 2, 1)
    q_new = q_t.reshape(3, rank, hidden).transpose(0, 2, 1)
    return token_grad, new_error, p_hat, q_new


def solution(mesh):
    return jax.shard_map(
        functools.partial(on_device, mesh.shape["node"], mesh.shape["grp"]),
        mesh=mesh,
        in_specs=(
            P(("node", "grp"), None),
            P(("node", "grp"), None),
            P("node", None),
            P("node", None),
            P("node", None),
            P("grp", "node", None),
            P(),
        ),
        out_specs=(P(("node", "grp"), None), P("grp", "node", None), P(None, "node", None), P()),
        check_vma=False,
    )
```

```python
import functools
import math

import jax
import jax.numpy as jnp
from jax import lax
from jax.experimental import pallas as pl
from jax.experimental.pallas import tpu as pltpu
from jax.sharding import PartitionSpec as P

MESH = pl.DeviceIdType.MESH
F32, BF16 = jnp.float32, jnp.bfloat16
HIGHEST = lax.Precision.HIGHEST
AHEAD, LAG = 2, 2
LANES = 128


def gelu_parts(value):
    coeff = math.sqrt(2.0 / math.pi)
    square = value * value
    tanh_value = jnp.tanh(coeff * (value + 0.044715 * square * value))
    activation = 0.5 * value * (1.0 + tanh_value)
    slope = 0.5 * (1.0 + tanh_value) + 0.5 * value * (1.0 - tanh_value * tanh_value) * coeff * (
        1.0 + 3.0 * 0.044715 * square
    )
    return activation, slope


def dot(a, b, precision=None):
    return jnp.dot(a, b, preferred_element_type=F32, precision=precision)


def dot_nt(a, b, precision=None):
    return lax.dot_general(
        a, b, (((1,), (1,)), ((), ())), preferred_element_type=F32, precision=precision
    )


def subsets(items):
    found = [()]
    for item in items:
        found += [s + (item,) for s in found]
    return found


def kernel(
    n, g, rank,
    tok_hbm, cot_hbm, w_gate, w_up, w_down, err_hbm, q_hbm,
    tok_grad, new_err, p_out, q_out,
    full, tok, cot, turned, turned_in, acts, mine_hid, their_hid, mine_back,
    their_back, grads, *rest
):
    bits = n.bit_length() - 1
    recv_bufs = rest[:bits - 1]
    (high, low, q_right, err, q_rows, tok_out, err_out, pw_acc, power, block_diag, q_t, pw_all,
     gram_all, q_part, q_rs, q_grp, q_all, send_sems, recv_sems, local_sems) = rest[bits - 1:]
    me, grp = lax.axis_index("node"), lax.axis_index("grp")
    rows, hidden = w_gate.shape
    tokens, depth = tok.shape
    side = depth // 2
    wide = 2 * LANES
    chunks = hidden // wide
    blocks = hidden // LANES
    used = 3 * rank
    weights = (w_gate, w_up, w_down)

    barrier = pltpu.get_barrier_semaphore()
    for d in range(1, n):
        pl.semaphore_signal(barrier, inc=1, device_id=(lax.rem(me + d, n), grp), device_id_type=MESH)
    for d in range(1, g):
        pl.semaphore_signal(barrier, inc=1, device_id=(me, lax.rem(grp + d, g)), device_id_type=MESH)

    flip = [(1 << b) * (1 - 2 * lax.rem(me // (1 << b), 2)) for b in range(bits)]
    offset = lambda mask: sum((flip[b] for b in mask), 0)
    pair = me + flip[0]
    core = lax.rem(me, 2)
    half_node = me // 2
    half_flip = [0] + [
        (1 << (b - 1)) * (1 - 2 * lax.rem(me // (1 << b), 2)) for b in range(1, bits)
    ]
    half_offset = lambda mask: sum((half_flip[b] for b in mask), 0)
    plane = lax.rem(grp, 2)
    twin = grp + 1 - 2 * plane
    outer = list(range(1, bits))
    orders = [outer, outer[::-1]]
    steps = len(outer)
    block = lambda index: pl.ds(pl.multiple_of(index * rows, rows), rows)

    def local(src, dst, index):
        copy = pltpu.make_async_copy(src, dst, local_sems.at[index])
        copy.start()
        return copy

    for c in range(chunks):
        for j in (2 * c, 2 * c + 1):
            for w in range(3):
                local(weights[w].at[:, pl.ds(j * LANES, LANES)], full.at[j, w, block(me)], c)
    cot_load = local(cot_hbm, cot, chunks)
    tok_load = local(tok_hbm, tok, chunks + 1)
    q_load = local(q_hbm, q_rows.at[0:used], chunks + 2)
    err_load = local(err_hbm.at[0], err, chunks + 3)

    arrive_index, leave_index, leave_refs = {}, {}, {}

    def send(src, dst, node, group, arrive, leave):
        pltpu.make_async_remote_copy(
            src_ref=src, dst_ref=dst,
            send_sem=send_sems.at[leave_index.setdefault(leave, len(leave_index))],
            recv_sem=recv_sems.at[arrive_index.setdefault(arrive, len(arrive_index))],
            device_id=(node, group), device_id_type=MESH,
        ).start()

    def whole(ref, arrive, leave):
        return pltpu.make_async_remote_copy(
            src_ref=ref, dst_ref=ref,
            send_sem=send_sems.at[leave_index[leave]], recv_sem=recv_sems.at[arrive_index[arrive]],
            device_id=(me, twin), device_id_type=MESH,
        )

    def wait_all(ref, arrive, leave):
        leave_refs.setdefault(leave, (ref, arrive))
        whole(ref, arrive, leave).wait_recv()

    if rows % 32 == 0:
        parts = [[(0, rows // 2, 0), (rows // 2, rows // 2, 1)]] * chunks
    else:
        parts = [[(0, rows, c % 2)] for c in range(chunks)]

    def piece(j, mask, part):
        start = (me + offset(mask)) * rows + part[0]
        return full.at[j, :, pl.ds(pl.multiple_of(start, math.gcd(rows, part[1])), part[1]), :]

    def column_block(side_of, c):
        return 2 * c + (plane if side_of == 0 else 1 - plane)

    def new_masks(t, order):
        return [mask + (order[t],) for mask in subsets(order[:t])]

    def gather_send(c, t, part):
        order = orders[part[2]]
        for mask in subsets(order[:t]):
            at = piece(2 * c + plane, mask, part)
            send(at, at, me + flip[order[t]], grp, ("plane", c, t, part), "plane")

    def gather_step(c, t):
        for part in parts[c]:
            wait_all(full.at[2 * c, :, 0:part[1] << t, :], ("plane", c, t, part), "plane")
            if t + 1 < steps:
                gather_send(c, t + 1, part)
            for mask in new_masks(t, orders[part[2]]):
                at = piece(2 * c + plane, mask, part)
                send(at, at, me, twin, ("twin", c, t), "twin")
                send(at, at, pair, grp, ("pair", 0, c), "pair")

    def relay(c):
        for t in range(steps):
            wait_all(full.at[2 * c, :, 0:rows << t, :], ("twin", c, t), "twin")
            for part in parts[c]:
                for mask in new_masks(t, orders[part[2]]):
                    at = piece(2 * c + 1 - plane, mask, part)
                    send(at, at, pair, grp, ("pair", 1, c), "pair")

    pl.semaphore_wait(barrier, n - 1 + g - 1)

    def launch(c):
        at = full.at[pl.ds(2 * c, 2), :, block(me), :]
        pltpu.make_async_copy(at, at, local_sems.at[c]).wait()
        for part in parts[c]:
            gather_send(c, 0, part)
        for side_of in range(2):
            at = full.at[column_block(side_of, c), :, block(me), :]
            send(at, at, pair, grp, ("pair", side_of, c), "pair")

    for c in range(min(2, chunks)):
        launch(c)

    pw_acc[...] = jnp.zeros_like(pw_acc)
    power[...] = jnp.zeros_like(power)
    block_diag[...] = jnp.zeros_like(block_diag)
    q_t[...] = jnp.zeros_like(q_t)
    for buf in (high, low):
        for m in range(3):
            for j in range(blocks):
                buf[m, j, rows:, :] = jnp.zeros((buf.shape[2] - rows, LANES), BF16)

    def turn(which, i):
        src = (tok, cot)[which]
        tile = src[:, i * wide:(i + 1) * wide].T
        first = i * wide
        while first < (i + 1) * wide:
            b = first // rows
            last = min((b + 1) * rows, (i + 1) * wide)
            at = (b // 2) * rows + first - b * rows
            turned[which, b % 2, at:at + last - first, :] = tile[first - i * wide:last - i * wide]
            first = last

    def right_factors():
        q_load.wait()
        q_rows[used:, :] = jnp.zeros((LANES - used, hidden), F32)
        lane = lax.broadcasted_iota(jnp.int32, (wide, LANES), 1)
        for c in range(chunks):
            at = slice(c * wide, (c + 1) * wide)
            columns = q_rows[:, at].T
            top = columns.astype(BF16)
            bottom = (columns - top.astype(F32)).astype(BF16)
            for m in range(3):
                inside_m = (lane >= m * rank) & (lane < (m + 1) * rank)
                q_right[m, at, 0:LANES] = jnp.where(inside_m, top.astype(F32), 0.0).astype(BF16)
                q_right[m, at, LANES:] = jnp.where(inside_m, bottom.astype(F32), 0.0).astype(BF16)

    filler = []
    for which, load in ((1, cot_load), (0, tok_load)):
        filler.append(load.wait)
        for i in range(depth // wide):
            filler.append(functools.partial(turn, which, i))
        filler.append(functools.partial(
            send, turned.at[which, 1 - core], turned_in.at[which], pair, grp, "turned", "turned"))
    filler.append(right_factors)

    def forward(j):
        both = dot(tok[...], jnp.concatenate([full[j, 0], full[j, 1]], axis=1))
        acts[...] = both
        up_pre = acts[:, LANES:]
        activation, slope = gelu_parts(acts[:, 0:LANES])
        mine_hid[j] = (activation * up_pre).astype(BF16)
        acts[:, LANES:] = activation
        acts[:, 0:LANES] = up_pre * slope

    def backward(j):
        back = dot(cot[...], full[j, 2])
        mine_back[j, :, 0:LANES] = (back * acts[:, 0:LANES]).astype(BF16)
        mine_back[j, :, LANES:] = (back * acts[:, LANES:]).astype(BF16)

    tile = side // 2
    group_m = ((2,), (0, 1))

    def gradient(u, j, k):
        own, other = ((mine_hid, their_hid), (mine_back, their_back))[k]
        right = jnp.concatenate([own[j], other[j]], axis=0)
        for i in range(2):
            at = pl.ds(i * tile, tile)
            left = jnp.concatenate([turned[1 - k, core, at, :], turned_in[1 - k, at, :]], axis=1)
            part = dot(left, right).astype(BF16)
            for i, m in enumerate(group_m[k]):
                grads[u, m, at, :] = part[:, i * LANES:(i + 1) * LANES]

    slots_of = {2: 0, 0: 1, 1: 2}

    def reduce_start(u, k, t):
        for m in group_m[k]:
            for first, size, h in parts[u % chunks]:
                bit = orders[h][t]
                for slot, mask in enumerate(subsets(orders[h][t + 1:])):
                    at = half_node + half_flip[bit] + half_offset(mask)
                    at = pl.ds(pl.multiple_of(at * rows + first, math.gcd(rows, size)), size)
                    dst = recv_bufs[t].at[u * 3 + slots_of[m], slot, pl.ds(first, size)]
                    send(grads.at[u, m, at], dst, me + flip[bit], grp,
                         ("reduce", u, k, t), ("reduce", t))

    scale = 1.0 / math.sqrt(tokens * n)

    def reduce_add(u, j, k, t):
        wait_all(
            recv_bufs[t].at[pl.ds(u * 3 + k, 1 + k)], ("reduce", u, k, t), ("reduce", t))
        for m in group_m[k]:
            for first, size, h in parts[u % chunks]:
                for slot, mask in enumerate(subsets(orders[h][t + 1:])):
                    at = (half_node + half_offset(mask)) * rows + first
                    at = pl.ds(pl.multiple_of(at, math.gcd(rows, size)), size)
                    total = (
                        grads[u, m, at, :].astype(F32)
                        + recv_bufs[t][u * 3 + slots_of[m], slot, first:first + size].astype(F32)
                    )
                    if t < steps - 1:
                        grads[u, m, at, :] = total.astype(BF16)
                    else:
                        span = pl.ds(pl.multiple_of(m * hidden + j * LANES, LANES), LANES)
                        memory = err[first:first + size, span].astype(F32)
                        merged = total * scale + memory
                        top = merged.astype(BF16)
                        high[m, j, first:first + size] = top
                        low[m, j, first:first + size] = (merged - top.astype(F32)).astype(BF16)

    def reduce_finish(u, j, k):
        reduce_add(u, j, k, steps - 1)
        at = pl.ds(pl.multiple_of(j * LANES, LANES), LANES)
        for m in group_m[k]:
            both = dot(high[m, j, 0:rows], q_right[m, at, :])
            rest_part = dot(low[m, j, 0:rows], q_right[m, at, 0:LANES])
            pw_acc[...] += both[:, 0:LANES] + both[:, LANES:] + rest_part

    def token_part(i):
        at = slice(i * wide, (i + 1) * wide)
        total = jnp.zeros((tokens, wide), F32)
        for k in range(2):
            lanes_k = slice(k * LANES, (k + 1) * LANES)
            left = jnp.concatenate([mine_back[j, :, lanes_k] for j in range(blocks)], axis=1)
            right = jnp.concatenate([full[j, k, at, :] for j in range(blocks)], axis=1)
            total += dot_nt(left, right)
        tok_out[:, at] = total.astype(BF16)
        local(tok_out.at[:, at], tok_grad.at[:, at], chunks + 4)

    token_tiles = list(range(depth // wide))

    def token_work(amount):
        for _ in range(min(amount, len(token_tiles))):
            token_part(token_tiles.pop(0))

    units = [(0, c) for c in range(chunks)]
    for c in range(chunks):
        units.insert(min(chunks - 1 + 2 * c, len(units)), (1, c))

    def prepare(u):
        side_of, c = units[u]
        wait_all(full.at[2 * c, :, 0:side, :], ("pair", side_of, c), "pair")
        j = column_block(*units[u])
        forward(j)
        send(mine_hid.at[j], their_hid.at[j], pair, grp, ("hidden", u), "hidden")
        backward(j)
        send(mine_back.at[j], their_back.at[j], pair, grp, ("back", u), "back")

    def reduce_all(u):
        j = column_block(*units[u])
        wait_all(their_hid.at[j], ("hidden", u), "hidden")
        gradient(u, j, 0)
        reduce_start(u, 0, 0)
        wait_all(their_back.at[j], ("back", u), "back")
        gradient(u, j, 1)
        reduce_start(u, 1, 0)

    def advance(u, t):
        j = column_block(*units[u])
        for k in range(2):
            reduce_add(u, j, k, t - 1)
            reduce_start(u, k, t)

    def finish(u):
        j = column_block(*units[u])
        for k in range(2):
            reduce_finish(u, j, k)

    events = sorted(
        ((c, t) for c in range(chunks) for t in range(steps)), key=lambda e: (2 * e[1] + e[0], -e[1])
    )
    ready = [i for i, (_, t) in enumerate(events) if t == steps - 1]
    each = -(-len(filler) // (ready[0] + 1))
    last = len(units) - 1
    done_u, relayed = [0], [0]

    def front():
        if done_u[0] == 0:
            err_load.wait()
            wait_all(turned_in, "turned", "turned")
        reduce_all(done_u[0])
        done_u[0] += 1

    for i, (c, t) in enumerate(events):
        for work in filler[:each]:
            work()
        filler = filler[each:]
        if i == len(events) - 1:
            relay(0)
            relayed[0] += 1
        gather_step(c, t)
        if t == 0 and c + 2 < chunks:
            launch(c + 2)
        if i > ready[0]:
            if t == steps - 1:
                front()
            if t < steps - 1 or c == chunks - 1:
                continue
        if t == steps - 1:
            prepare(done_u[0])
    behind = [0]

    def settle(tokens_beside=0):
        u = behind[0]
        for t in range(1, steps):
            advance(u, t)
        token_work(tokens_beside)
        if u >= LAG:
            finish(u - LAG)
        behind[0] += 1

    while done_u[0] <= last:
        ahead = done_u[0]
        prepare(ahead)
        front()
        if ahead < last and units[ahead + 1][0] and relayed[0] < chunks:
            relay(relayed[0])
            relayed[0] += 1
        while behind[0] <= ahead - AHEAD:
            settle()
    while behind[0] <= last:
        settle(3)
    token_work(len(token_tiles))
    for u in range(max(last + 1 - LAG, 0), last + 1):
        finish(u)

    pw_all[grp] = pw_acc[...].astype(BF16)
    for d in range(1, g):
        send(pw_all.at[grp], pw_all.at[grp], me, lax.rem(grp + d, g), "power", "power")
    wait_all(pw_all.at[0:g - 1], "power", "power")
    total = pw_all[0].astype(F32)
    for k in range(1, g):
        total += pw_all[k].astype(F32)
    power[0:rows, :] = total * (1.0 / g)

    lane = lax.broadcasted_iota(jnp.int32, (rank, LANES), 1)
    row = lax.broadcasted_iota(jnp.int32, (rank, LANES), 0)
    padded = power[...]
    gram = dot(padded.T, padded, HIGHEST)
    picked = gram[0:rank]
    for m in range(1, 3):
        picked = jnp.where(lane >= m * rank, gram[m * rank:(m + 1) * rank], picked)
    gram_all[me] = picked
    for d in range(1, n):
        send(gram_all.at[me], gram_all.at[me], lax.rem(me + d, n), grp, "gram", "gram")
    wait_all(gram_all.at[0:n - 1], "gram", "gram")
    picked = gram_all[0]
    for k in range(1, n):
        picked += gram_all[k]

    work = []
    for m in range(3):
        rolled = picked if m == 0 else pltpu.roll(picked, LANES - m * rank, 1)
        unit = jnp.where(lane == row + rank, 1.0, 0.0).astype(F32)
        work.append(jnp.where(lane < rank, rolled, unit))
    for j in range(rank):
        for m in range(3):
            a = work[m]
            inverse = 1.0 / jnp.sqrt(a[j:j + 1, j:j + 1])
            pivot_row = a[j:j + 1, :] * inverse
            column = a[:, j:j + 1] * inverse
            work[m] = jnp.where(row > j, a - column * pivot_row, jnp.where(row == j, pivot_row, a))
    for m in range(3):
        shift = ((m - 1) * rank) % LANES
        moved = work[m] if shift == 0 else pltpu.roll(work[m], shift, 1)
        inside_m = (lane >= m * rank) & (lane < (m + 1) * rank)
        block_diag[m * rank:(m + 1) * rank, :] = jnp.where(inside_m, moved, 0.0)
    hat_t = dot_nt(block_diag[...], power[...], HIGHEST)
    hat = dot_nt(power[0:rows, :], block_diag[...], HIGHEST)
    p_out[...] = hat_t[0:used, 0:rows]

    c_blocks = min(n, hidden // LANES)
    r_blocks = n // c_blocks
    c_size, r_size = hidden // c_blocks, used // r_blocks
    hat_top = hat_t.astype(BF16)
    hat_bottom = (hat_t - hat_top.astype(F32)).astype(BF16)
    for m in range(3):
        at = slice(m * rank, (m + 1) * rank)
        left = jnp.concatenate([hat_top[at], hat_bottom[at]], axis=0)
        both = dot(left, jnp.concatenate([high[m, j] for j in range(blocks)], axis=1))
        q_t[at, :] = both[0:rank] + both[rank:]
    spots = [
        (slice(c // c_blocks * r_size, (c // c_blocks + 1) * r_size),
         slice(c % c_blocks * c_size, (c % c_blocks + 1) * c_size))
        for c in range(n)
    ]
    for c in range(n):
        q_part[c] = q_t[spots[c]].astype(BF16)
    q_rs[me] = q_part[me]
    for d in range(1, n):
        to = lax.rem(me + d, n)
        send(q_part.at[to], q_rs.at[me], to, grp, "term", "term")
    wait_all(q_rs.at[0:n - 1], "term", "term")
    total = q_rs[0].astype(F32)
    for k in range(1, n):
        total += q_rs[k].astype(F32)
    q_grp[grp] = total.astype(BF16)
    for d in range(1, g):
        send(q_grp.at[grp], q_grp.at[grp], me, lax.rem(grp + d, g), "group", "group")
    wait_all(q_grp.at[0:g - 1], "group", "group")
    total = q_grp[0].astype(F32)
    for k in range(1, g):
        total += q_grp[k].astype(F32)
    q_all[me] = (total * (1.0 / g)).astype(BF16)
    for d in range(1, n):
        send(q_all.at[me], q_all.at[me], lax.rem(me + d, n), grp, "right", "right")
    wait_all(q_all.at[0:n - 1], "right", "right")
    for c in range(n):
        q_t[spots[c]] = q_all[c].astype(F32)
    q_out[...] = q_t[0:used, :]

    lanes = lax.broadcasted_iota(jnp.int32, (rows, LANES), 1)
    right = q_t[...].astype(BF16)
    right = jnp.concatenate([right, right], axis=0)
    for m in range(3):
        own = jnp.where((lanes >= m * rank) & (lanes < (m + 1) * rank), hat, 0.0)
        top = own.astype(BF16)
        left = jnp.concatenate([top, (own - top.astype(F32)).astype(BF16)], axis=1)
        for c in range(chunks):
            at = slice(c * wide, (c + 1) * wide)
            rebuilt = dot(left, right[:, at])
            merged = jnp.concatenate([
                high[m, j, 0:rows].astype(F32) + low[m, j, 0:rows].astype(F32)
                for j in (2 * c, 2 * c + 1)
            ], axis=1)
            err_out[:, m * hidden + c * wide:m * hidden + (c + 1) * wide] = (
                merged - rebuilt
            ).astype(BF16)
        at = pl.ds(m * hidden, hidden)
        local(err_out.at[:, at], new_err.at[0, :, at], chunks + 5)
    others = n // 2 - 1
    leave_refs["plane"] = (full.at[0:chunks, :, 0:others * rows, :], leave_refs["plane"][1])
    leave_refs["twin"] = (leave_refs["plane"][0], leave_refs["twin"][1])
    leave_refs["pair"] = (full.at[0:chunks], leave_refs["pair"][1])
    for t in range(steps):
        leave_refs["reduce", t] = (recv_bufs[t], leave_refs["reduce", t][1])
    leave_refs["hidden"] = (their_hid, leave_refs["hidden"][1])
    leave_refs["back"] = (their_back, leave_refs["back"][1])
    for leave, (ref, arrive) in leave_refs.items():
        whole(ref, arrive, leave).wait_send()
    pltpu.make_async_copy(tok_out, tok_grad, local_sems.at[chunks + 4]).wait()
    pltpu.make_async_copy(err_out, new_err.at[0], local_sems.at[chunks + 5]).wait()


def write_results(*refs):
    ins, outs, bufs, sems = refs[:4], refs[4:8], refs[8:12], refs[12]
    cuts = []
    for k in (0, 1, 2, 3):
        axis = len(ins[k].shape) - 2
        size = ins[k].shape[axis]
        count = 3 if k == 0 else 2 if k == 1 else 1
        for i in range(count):
            at = (slice(None),) * axis + (pl.ds(i * (size // count), size // count),)
            cuts.append((k, at))
    reads, writes = [], []
    for i, (k, at) in enumerate(cuts):
        reads.append(pltpu.make_async_copy(ins[k].at[at], bufs[k].at[at], sems.at[0, i]))
        reads[-1].start()
    for i, (k, at) in enumerate(cuts):
        reads[i].wait()
        writes.append(pltpu.make_async_copy(bufs[k].at[at], outs[k].at[at], sems.at[1, i]))
        writes[-1].start()
    for copy in writes:
        copy.wait()


def on_device(n, g, tokens, cotangent, gate_weight, up_weight, down_weight_t, error_memory, q_init):
    token_rows, depth = tokens.shape
    rows, hidden = gate_weight.shape
    rank = q_init.shape[2]
    used = 3 * rank
    bits = n.bit_length() - 1
    side = depth // 2
    wide = 2 * LANES
    chunks = hidden // wide
    blocks = hidden // LANES
    padded = -(-rows // LANES) * LANES
    q_rows = q_init.transpose(0, 2, 1).reshape(used, hidden)
    c_blocks = min(n, hidden // LANES)
    chunk = (used // (n // c_blocks), hidden // c_blocks)
    parts = 2 if rows % 32 == 0 else 1
    arrivals = (
        chunks * (bits - 1) * (parts + 1) + blocks + 2 * blocks * (bits - 1) + 2 * blocks + 6
    )
    leaves = 11 + bits - 1
    recv_shapes = [
        pltpu.VMEM((blocks * 3, 1 << (bits - 2 - t), rows, LANES), BF16) for t in range(bits - 1)
    ]
    vmem = pl.BlockSpec(memory_space=pltpu.VMEM)
    hbm = pl.BlockSpec(memory_space=pl.ANY)
    token_grad, new_error, hat_t, q_t = pl.pallas_call(
        functools.partial(kernel, n, g, rank),
        out_shape=(
            jax.ShapeDtypeStruct((token_rows, depth), BF16),
            jax.ShapeDtypeStruct((1, rows, 3 * hidden), BF16),
            jax.ShapeDtypeStruct((used, rows), F32),
            jax.ShapeDtypeStruct((used, hidden), F32),
        ),
        in_specs=[hbm] * 7,
        out_specs=(hbm, hbm, vmem, vmem),
        scratch_shapes=[
            pltpu.VMEM((2 * chunks, 3, depth, LANES), BF16),
            pltpu.VMEM((token_rows, depth), BF16),
            pltpu.VMEM((token_rows, depth), BF16),
            pltpu.VMEM((2, 2, side, token_rows), BF16),
            pltpu.VMEM((2, side, token_rows), BF16),
            pltpu.VMEM((token_rows, wide), F32),
            pltpu.VMEM((blocks, token_rows, LANES), BF16),
            pltpu.VMEM((blocks, token_rows, LANES), BF16),
            pltpu.VMEM((blocks, token_rows, wide), BF16),
            pltpu.VMEM((blocks, token_rows, wide), BF16),
            pltpu.VMEM((blocks, 3, side, LANES), BF16),
            *recv_shapes,
            pltpu.VMEM((3, blocks, padded, LANES), BF16),
            pltpu.VMEM((3, blocks, padded, LANES), BF16),
            pltpu.VMEM((3, hidden, wide), BF16),
            pltpu.VMEM((rows, 3 * hidden), BF16),
            pltpu.VMEM((LANES, hidden), F32),
            pltpu.VMEM((token_rows, depth), BF16),
            pltpu.VMEM((rows, 3 * hidden), BF16),
            pltpu.VMEM((rows, LANES), F32),
            pltpu.VMEM((padded, LANES), F32),
            pltpu.VMEM((LANES, LANES), F32),
            pltpu.VMEM((LANES, hidden), F32),
            pltpu.VMEM((g, rows, LANES), BF16),
            pltpu.VMEM((n, rank, LANES), F32),
            pltpu.VMEM((n,) + chunk, BF16),
            pltpu.VMEM((n,) + chunk, BF16),
            pltpu.VMEM((g,) + chunk, BF16),
            pltpu.VMEM((n,) + chunk, BF16),
            pltpu.SemaphoreType.DMA((leaves,)),
            pltpu.SemaphoreType.DMA((arrivals,)),
            pltpu.SemaphoreType.DMA((chunks + 6,)),
        ],
        compiler_params=pltpu.CompilerParams(
            collective_id=0, has_side_effects=True, vmem_limit_bytes=67_043_328
        ),
    )(tokens, cotangent, gate_weight, up_weight, down_weight_t, error_memory, q_rows)
    results = (token_grad, new_error, hat_t, q_t)
    token_grad, new_error, hat_t, q_t = pl.pallas_call(
        write_results,
        out_shape=tuple(jax.ShapeDtypeStruct(r.shape, r.dtype) for r in results),
        in_specs=[hbm] * 4,
        out_specs=(hbm,) * 4,
        scratch_shapes=[
            *(pltpu.VMEM(r.shape, r.dtype) for r in results),
            pltpu.SemaphoreType.DMA((2, 8)),
        ],
    )(*results)
    p_hat = hat_t.reshape(3, rank, rows).transpose(0, 2, 1)
    q_new = q_t.reshape(3, rank, hidden).transpose(0, 2, 1)
    return token_grad, new_error, p_hat, q_new


def solution(mesh):
    return jax.shard_map(
        functools.partial(on_device, mesh.shape["node"], mesh.shape["grp"]),
        mesh=mesh,
        in_specs=(
            P(("node", "grp"), None),
            P(("node", "grp"), None),
            P("node", None),
            P("node", None),
            P("node", None),
            P("grp", "node", None),
            P(),
        ),
        out_specs=(P(("node", "grp"), None), P("grp", "node", None), P(None, "node", None), P()),
        check_vma=False,
    )
```

```python
import functools
import math

import jax
import jax.numpy as jnp
from jax import lax
from jax.experimental import pallas as pl
from jax.experimental.pallas import tpu as pltpu
from jax.sharding import PartitionSpec as P

MESH = pl.DeviceIdType.MESH
F32, BF16 = jnp.float32, jnp.bfloat16
HIGHEST = lax.Precision.HIGHEST
AHEAD, LAG, PIVOTS = 2, 4, 4
LANES = 128


def gelu_parts(value):
    coeff = math.sqrt(2.0 / math.pi)
    square = value * value
    tanh_value = jnp.tanh(coeff * (value + 0.044715 * square * value))
    activation = 0.5 * value * (1.0 + tanh_value)
    slope = 0.5 * (1.0 + tanh_value) + 0.5 * value * (1.0 - tanh_value * tanh_value) * coeff * (
        1.0 + 3.0 * 0.044715 * square
    )
    return activation, slope


def dot(a, b, precision=None):
    return jnp.dot(a, b, preferred_element_type=F32, precision=precision)


def dot_nt(a, b, precision=None):
    return lax.dot_general(
        a, b, (((1,), (1,)), ((), ())), preferred_element_type=F32, precision=precision
    )


def subsets(items):
    found = [()]
    for item in items:
        found += [s + (item,) for s in found]
    return found


def kernel(
    n, g, rank,
    tok_hbm, cot_hbm, w_gate, w_up, w_down, err_hbm, q_hbm,
    tok_grad, new_err, p_out, q_out,
    full, tok, cot, turned, turned_in, acts, mine_hid, their_hid, mine_back,
    their_back, grads, *rest
):
    bits = n.bit_length() - 1
    recv_bufs = rest[:bits - 1]
    (high, low, q_right, err, q_rows, tok_out, err_out, hat_out, early, pw_acc, power, block_diag, q_t, pw_all,
     gram_all, q_part, q_rs, q_grp, q_all, send_sems, recv_sems, local_sems) = rest[bits - 1:]
    me, grp = lax.axis_index("node"), lax.axis_index("grp")
    rows, hidden = w_gate.shape
    tokens, depth = tok.shape
    side = depth // 2
    wide = 2 * LANES
    chunks = hidden // wide
    blocks = hidden // LANES
    used = 3 * rank
    weights = (w_gate, w_up, w_down)

    barrier = pltpu.get_barrier_semaphore()
    for d in range(1, n):
        pl.semaphore_signal(barrier, inc=1, device_id=(lax.rem(me + d, n), grp), device_id_type=MESH)
    for d in range(1, g):
        pl.semaphore_signal(barrier, inc=1, device_id=(me, lax.rem(grp + d, g)), device_id_type=MESH)

    flip = [(1 << b) * (1 - 2 * lax.rem(me // (1 << b), 2)) for b in range(bits)]
    offset = lambda mask: sum((flip[b] for b in mask), 0)
    pair = me + flip[0]
    core = lax.rem(me, 2)
    half_node = me // 2
    half_flip = [0] + [
        (1 << (b - 1)) * (1 - 2 * lax.rem(me // (1 << b), 2)) for b in range(1, bits)
    ]
    half_offset = lambda mask: sum((half_flip[b] for b in mask), 0)
    plane = lax.rem(grp, 2)
    twin = grp + 1 - 2 * plane
    outer = list(range(1, bits))
    orders = [outer, outer[::-1]]
    steps = len(outer)
    block = lambda index: pl.ds(pl.multiple_of(index * rows, rows), rows)

    def local(src, dst, index):
        copy = pltpu.make_async_copy(src, dst, local_sems.at[index])
        copy.start()
        return copy

    for c in range(chunks):
        for j in (2 * c, 2 * c + 1):
            for w in range(3):
                local(weights[w].at[:, pl.ds(j * LANES, LANES)], full.at[j, w, block(me)], c)
    cot_load = local(cot_hbm, cot, chunks)
    tok_load = local(tok_hbm, tok, chunks + 1)
    q_load = local(q_hbm, q_rows.at[0:used], chunks + 2)
    err_load = local(err_hbm.at[0], err, chunks + 3)

    arrive_index, leave_index, leave_refs = {}, {}, {}

    def send(src, dst, node, group, arrive, leave):
        pltpu.make_async_remote_copy(
            src_ref=src, dst_ref=dst,
            send_sem=send_sems.at[leave_index.setdefault(leave, len(leave_index))],
            recv_sem=recv_sems.at[arrive_index.setdefault(arrive, len(arrive_index))],
            device_id=(node, group), device_id_type=MESH,
        ).start()

    def whole(ref, arrive, leave):
        return pltpu.make_async_remote_copy(
            src_ref=ref, dst_ref=ref,
            send_sem=send_sems.at[leave_index[leave]], recv_sem=recv_sems.at[arrive_index[arrive]],
            device_id=(me, twin), device_id_type=MESH,
        )

    def wait_all(ref, arrive, leave):
        leave_refs.setdefault(leave, (ref, arrive))
        whole(ref, arrive, leave).wait_recv()

    if rows % 32 == 0:
        parts = [[(0, rows // 2, 0), (rows // 2, rows // 2, 1)]] * chunks
    else:
        parts = [[(0, rows, c % 2)] for c in range(chunks)]

    def piece(j, mask, part):
        start = (me + offset(mask)) * rows + part[0]
        return full.at[j, :, pl.ds(pl.multiple_of(start, math.gcd(rows, part[1])), part[1]), :]

    def column_block(side_of, c):
        return 2 * c + (plane if side_of == 0 else 1 - plane)

    def new_masks(t, order):
        return [mask + (order[t],) for mask in subsets(order[:t])]

    def gather_send(c, t, part):
        order = orders[part[2]]
        for mask in subsets(order[:t]):
            at = piece(2 * c + plane, mask, part)
            send(at, at, me + flip[order[t]], grp, ("plane", c, t, part), "plane")

    def gather_step(c, t):
        for part in parts[c]:
            wait_all(full.at[2 * c, :, 0:part[1] << t, :], ("plane", c, t, part), "plane")
            if t + 1 < steps:
                gather_send(c, t + 1, part)
            for mask in new_masks(t, orders[part[2]]):
                at = piece(2 * c + plane, mask, part)
                send(at, at, me, twin, ("twin", c, t), "twin")
                send(at, at, pair, grp, ("pair", 0, c), "pair")

    def relay(c):
        for t in range(steps):
            wait_all(full.at[2 * c, :, 0:rows << t, :], ("twin", c, t), "twin")
            for part in parts[c]:
                for mask in new_masks(t, orders[part[2]]):
                    at = piece(2 * c + 1 - plane, mask, part)
                    send(at, at, pair, grp, ("pair", 1, c), "pair")

    pl.semaphore_wait(barrier, n - 1 + g - 1)

    def launch(c):
        at = full.at[pl.ds(2 * c, 2), :, block(me), :]
        pltpu.make_async_copy(at, at, local_sems.at[c]).wait()
        for part in parts[c]:
            gather_send(c, 0, part)
        for side_of in range(2):
            at = full.at[column_block(side_of, c), :, block(me), :]
            send(at, at, pair, grp, ("pair", side_of, c), "pair")

    for c in range(min(2, chunks)):
        launch(c)

    pw_acc[...] = jnp.zeros_like(pw_acc)
    early[...] = jnp.zeros_like(early)
    power[...] = jnp.zeros_like(power)
    block_diag[...] = jnp.zeros_like(block_diag)
    q_t[...] = jnp.zeros_like(q_t)
    for buf in (high, low):
        for m in range(3):
            for j in range(blocks):
                buf[m, j, rows:, :] = jnp.zeros((buf.shape[2] - rows, LANES), BF16)

    def turn(which, i):
        src = (tok, cot)[which]
        tile = src[:, i * wide:(i + 1) * wide].T
        first = i * wide
        while first < (i + 1) * wide:
            b = first // rows
            last = min((b + 1) * rows, (i + 1) * wide)
            at = (b // 2) * rows + first - b * rows
            turned[which, b % 2, at:at + last - first, :] = tile[first - i * wide:last - i * wide]
            first = last

    def right_factors():
        q_load.wait()
        q_rows[used:, :] = jnp.zeros((LANES - used, hidden), F32)
        lane = lax.broadcasted_iota(jnp.int32, (wide, LANES), 1)
        for c in range(chunks):
            at = slice(c * wide, (c + 1) * wide)
            columns = q_rows[:, at].T
            top = columns.astype(BF16)
            bottom = (columns - top.astype(F32)).astype(BF16)
            for m in range(3):
                inside_m = (lane >= m * rank) & (lane < (m + 1) * rank)
                q_right[m, at, 0:LANES] = jnp.where(inside_m, top.astype(F32), 0.0).astype(BF16)
                q_right[m, at, LANES:] = jnp.where(inside_m, bottom.astype(F32), 0.0).astype(BF16)

    units = [(0, c) for c in range(chunks)]
    for c in range(chunks):
        units.insert(min(chunks - 1 + 2 * c, len(units)), (1, c))
    extra = len(units)
    first_late = extra - (chunks - 1)

    def memory_power():
        err_load.wait()
        for side_of, c in units[first_late:]:
            j = column_block(side_of, c)
            at = pl.ds(pl.multiple_of(j * LANES, LANES), LANES)
            left = jnp.concatenate([
                err[:, pl.ds(pl.multiple_of(m * hidden + j * LANES, LANES), LANES)]
                for m in range(3)
            ], axis=1)
            both = dot(left, jnp.concatenate([q_right[m, at, :] for m in range(3)], axis=0))
            pw_acc[...] += both[:, 0:LANES] + both[:, LANES:]

    filler = []
    for which, load in ((1, cot_load), (0, tok_load)):
        filler.append(load.wait)
        for i in range(depth // wide):
            filler.append(functools.partial(turn, which, i))
        filler.append(functools.partial(
            send, turned.at[which, 1 - core], turned_in.at[which], pair, grp, "turned", "turned"))
    filler += [right_factors, memory_power]

    def forward(j):
        both = dot(tok[...], jnp.concatenate([full[j, 0], full[j, 1]], axis=1))
        acts[...] = both
        up_pre = acts[:, LANES:]
        activation, slope = gelu_parts(acts[:, 0:LANES])
        mine_hid[j] = (activation * up_pre).astype(BF16)
        acts[:, LANES:] = activation
        acts[:, 0:LANES] = up_pre * slope

    def backward(j):
        back = dot(cot[...], full[j, 2])
        mine_back[j, :, 0:LANES] = (back * acts[:, 0:LANES]).astype(BF16)
        mine_back[j, :, LANES:] = (back * acts[:, LANES:]).astype(BF16)

    tile = side // 2
    group_m = ((2,), (0, 1))

    def gradient(u, j, k):
        own, other = ((mine_hid, their_hid), (mine_back, their_back))[k]
        right = jnp.concatenate([own[j], other[j]], axis=0)
        for i in range(2):
            at = pl.ds(i * tile, tile)
            left = jnp.concatenate([turned[1 - k, core, at, :], turned_in[1 - k, at, :]], axis=1)
            part = dot(left, right).astype(BF16)
            for i, m in enumerate(group_m[k]):
                grads[u, m, at, :] = part[:, i * LANES:(i + 1) * LANES]

    slots_of = {2: 0, 0: 1, 1: 2}

    def reduce_start(u, k, t):
        for m in group_m[k]:
            for first, size, h in parts[u % chunks]:
                bit = orders[h][t]
                for slot, mask in enumerate(subsets(orders[h][t + 1:])):
                    at = half_node + half_flip[bit] + half_offset(mask)
                    at = pl.ds(pl.multiple_of(at * rows + first, math.gcd(rows, size)), size)
                    dst = recv_bufs[t].at[u * 3 + slots_of[m], slot, pl.ds(first, size)]
                    send(grads.at[u, m, at], dst, me + flip[bit], grp,
                         ("reduce", u, k, t), ("reduce", t))

    scale = 1.0 / math.sqrt(tokens * n)

    def reduce_add(u, j, k, t):
        wait_all(
            recv_bufs[t].at[pl.ds(u * 3 + k, 1 + k)], ("reduce", u, k, t), ("reduce", t))
        for m in group_m[k]:
            for first, size, h in parts[u % chunks]:
                for slot, mask in enumerate(subsets(orders[h][t + 1:])):
                    at = (half_node + half_offset(mask)) * rows + first
                    at = pl.ds(pl.multiple_of(at, math.gcd(rows, size)), size)
                    total = (
                        grads[u, m, at, :].astype(F32)
                        + recv_bufs[t][u * 3 + slots_of[m], slot, first:first + size].astype(F32)
                    )
                    if t < steps - 1:
                        grads[u, m, at, :] = total.astype(BF16)
                    elif u == extra:
                        pw_acc[first:first + size] += total * scale
                    else:
                        span = pl.ds(pl.multiple_of(m * hidden + j * LANES, LANES), LANES)
                        memory = err[first:first + size, span].astype(F32)
                        merged = total * scale + memory
                        top = merged.astype(BF16)
                        high[m, j, first:first + size] = top
                        low[m, j, first:first + size] = (merged - top.astype(F32)).astype(BF16)

    def reduce_finish(u, j, k):
        reduce_add(u, j, k, steps - 1)
        at = pl.ds(pl.multiple_of(j * LANES, LANES), LANES)
        for m in group_m[k] if u < first_late else ():
            both = dot(high[m, j, 0:rows], q_right[m, at, :])
            rest_part = dot(low[m, j, 0:rows], q_right[m, at, 0:LANES])
            pw_acc[...] += both[:, 0:LANES] + both[:, LANES:] + rest_part

    def token_part(i):
        at = slice(i * wide, (i + 1) * wide)
        total = jnp.zeros((tokens, wide), F32)
        for k in range(2):
            lanes_k = slice(k * LANES, (k + 1) * LANES)
            left = jnp.concatenate([mine_back[j, :, lanes_k] for j in range(blocks)], axis=1)
            right = jnp.concatenate([full[j, k, at, :] for j in range(blocks)], axis=1)
            total += dot_nt(left, right)
        tok_out[:, at] = total.astype(BF16)
        local(tok_out.at[:, at], tok_grad.at[:, at], chunks + 4)

    token_tiles = list(range(depth // wide))

    def token_work(amount):
        for _ in range(min(amount, len(token_tiles))):
            token_part(token_tiles.pop(0))


    def prepare(u):
        side_of, c = units[u]
        wait_all(full.at[2 * c, :, 0:side, :], ("pair", side_of, c), "pair")
        j = column_block(*units[u])
        forward(j)
        send(mine_hid.at[j], their_hid.at[j], pair, grp, ("hidden", u), "hidden")
        backward(j)
        send(mine_back.at[j], their_back.at[j], pair, grp, ("back", u), "back")

    def early_power(u, j, k):
        at = pl.ds(pl.multiple_of(j * LANES, LANES), LANES)
        right = jnp.concatenate([q_right[m, at, :] for m in group_m[k]], axis=0)
        for i in range(2):
            span = pl.ds(i * tile, tile)
            left = jnp.concatenate([grads[u, m, span, :] for m in group_m[k]], axis=1)
            both = dot(left, right)
            early[span, :] += both[:, 0:LANES] + both[:, LANES:]

    def reduce_all(u, sent):
        j = column_block(*units[u])
        wait_all(their_hid.at[j], ("hidden", u), "hidden")
        for k in range(2):
            if k == 1:
                wait_all(their_back.at[j], ("back", u), "back")
            gradient(u, j, k)
            if k in sent:
                reduce_start(u, k, 0)
            if u >= first_late:
                early_power(u, j, k)

    def advance(u, t):
        j = column_block(*units[u])
        for k in range(2):
            reduce_add(u, j, k, t - 1)
            reduce_start(u, k, t)

    def finish(u):
        j = column_block(*units[u])
        for k in range(2):
            reduce_finish(u, j, k)

    events = sorted(
        ((c, t) for c in range(chunks) for t in range(steps)), key=lambda e: (2 * e[1] + e[0], -e[1])
    )
    ready = [i for i, (_, t) in enumerate(events) if t == steps - 1]
    each = -(-len(filler) // (ready[0] + 1))
    last = len(units) - 1
    done_u, relayed = [0], [0]

    def front(sent=(0, 1)):
        if done_u[0] == 0:
            wait_all(turned_in, "turned", "turned")
        reduce_all(done_u[0], sent)
        done_u[0] += 1

    for i, (c, t) in enumerate(events):
        for work in filler[:each]:
            work()
        filler = filler[each:]
        if i == len(events) - 1:
            relay(0)
            relayed[0] += 1
        gather_step(c, t)
        if t == 0 and c + 2 < chunks:
            launch(c + 2)
        if i > ready[0]:
            if t == steps - 1:
                front()
            if t < steps - 1 or c == chunks - 1:
                continue
        if t == steps - 1:
            prepare(done_u[0])
    behind = [0]

    def settle():
        u = behind[0]
        for t in range(1, steps):
            advance(u, t)
        if u >= LAG:
            finish(u - LAG)
        behind[0] += 1

    while done_u[0] <= last:
        ahead = done_u[0]
        prepare(ahead)
        front((0, 1) if ahead < last - 1 else (0,) if ahead < last else ())
        if ahead < last and units[ahead + 1][0] and relayed[0] < chunks:
            relay(relayed[0])
            relayed[0] += 1
        while ahead < last and behind[0] <= ahead - AHEAD:
            settle()
    grads[extra, 2] = early[...].astype(BF16)
    reduce_start(extra, 0, 0)
    reduce_start(last - 1, 1, 0)
    for u in range(max(behind[0] - LAG, 0), first_late):
        finish(u)
    for t in range(1, steps):
        reduce_add(extra, 0, 0, t - 1)
        reduce_start(extra, 0, t)
    for u in range(behind[0], last - 1):
        for t in range(1, steps):
            advance(u, t)
    for k in range(2):
        reduce_start(last, k, 0)
    reduce_add(extra, 0, 0, steps - 1)

    packed = pw_all.shape[1] < rows
    if packed:
        head = pw_all.shape[1]
        spare = lax.broadcasted_iota(jnp.int32, (head, LANES), 1) >= used
        tail = pw_acc[head:, :]
        moved = jnp.concatenate(
            [pltpu.roll(tail, used - m * rank, 1) for m in range(3)], axis=0)
        pw_all[grp] = jnp.where(spare, moved, pw_acc[0:head, :]).astype(BF16)
    else:
        pw_all[grp] = pw_acc[...].astype(BF16)
    for d in range(1, g):
        send(pw_all.at[grp], pw_all.at[grp], me, lax.rem(grp + d, g), "power", "power")
    for t in range(1, steps):
        advance(last - 1, t)
    for u in range(first_late, last - 1):
        finish(u)
    token_work(len(token_tiles))
    wait_all(pw_all.at[0:g - 1], "power", "power")
    total = pw_all[0].astype(F32)
    for k in range(1, g):
        total += pw_all[k].astype(F32)
    total = total * (1.0 / g)
    if packed:
        short = rows - head
        spot = lax.broadcasted_iota(jnp.int32, (short, LANES), 1) // rank
        tail = jnp.zeros((short, LANES), F32)
        for m in range(3):
            back = pltpu.roll(total[m * short:(m + 1) * short], LANES - used + m * rank, 1)
            tail = jnp.where(spot == m, back, tail)
        power[0:head, :] = jnp.where(spare, 0.0, total)
        power[head:rows, :] = tail
    else:
        power[0:rows, :] = total

    lane = lax.broadcasted_iota(jnp.int32, (rank, LANES), 1)
    row = lax.broadcasted_iota(jnp.int32, (rank, LANES), 0)
    padded = power[...]
    gram = dot(padded.T, padded, HIGHEST)
    picked = gram[0:rank]
    for m in range(1, 3):
        picked = jnp.where(lane >= m * rank, gram[m * rank:(m + 1) * rank], picked)
    gram_all[me] = picked
    for d in range(1, n):
        send(gram_all.at[me], gram_all.at[me], lax.rem(me + d, n), grp, "gram", "gram")
    for t in range(1, steps):
        advance(last, t)
    finish(last - 1)
    wait_all(gram_all.at[0:n - 1], "gram", "gram")
    finish(last)
    picked = gram_all[0]
    for k in range(1, n):
        picked += gram_all[k]

    work = []
    for m in range(3):
        rolled = picked if m == 0 else pltpu.roll(picked, LANES - m * rank, 1)
        unit = jnp.where(lane == row + rank, 1.0, 0.0).astype(F32)
        work.append(jnp.where(lane < rank, rolled, unit))
    for first in range(0, rank, PIVOTS):
        for m in range(3):
            a = work[m]
            pivots = range(PIVOTS)
            spread = [
                jnp.broadcast_to(a[:, first + i:first + i + 1], (rank, LANES)) for i in pivots
            ]
            pivot_rows = [a[first + i:first + i + 1, :] for i in pivots]
            update = None
            for i in pivots:
                inverse = 1.0 / spread[i][first + i:first + i + 1, :]
                for k in range(i + 1, PIVOTS):
                    factor = spread[i][first + k:first + k + 1, :] * inverse
                    spread[k] -= spread[i] * factor
                    pivot_rows[k] -= pivot_rows[i] * factor
                term = spread[i] * (pivot_rows[i] * inverse)
                update = term if update is None else update + term
            a = jnp.where(row >= first + PIVOTS, a - update, a)
            for i in pivots:
                a = jnp.where(row == first + i, pivot_rows[i], a)
            work[m] = a
    for m in range(3):
        diagonal = jnp.sum(jnp.where(lane == row, work[m], 0.0), axis=1, keepdims=True)
        work[m] = work[m] * (1.0 / jnp.sqrt(diagonal))
    for m in range(3):
        shift = ((m - 1) * rank) % LANES
        moved = work[m] if shift == 0 else pltpu.roll(work[m], shift, 1)
        inside_m = (lane >= m * rank) & (lane < (m + 1) * rank)
        block_diag[m * rank:(m + 1) * rank, :] = jnp.where(inside_m, moved, 0.0)
    hat_t = dot_nt(block_diag[...], power[...], HIGHEST)
    hat = dot_nt(power[0:rows, :], block_diag[...], HIGHEST)
    hat_out[...] = hat_t[0:used, 0:rows]
    local(hat_out, p_out, chunks + 6)

    c_blocks = min(n, hidden // LANES)
    r_blocks = n // c_blocks
    c_size, r_size = hidden // c_blocks, used // r_blocks
    hat_top = hat_t.astype(BF16)
    hat_bottom = (hat_t - hat_top.astype(F32)).astype(BF16)
    for m in range(3):
        at = slice(m * rank, (m + 1) * rank)
        left = jnp.concatenate([hat_top[at], hat_bottom[at]], axis=0)
        both = dot(left, jnp.concatenate([high[m, j] for j in range(blocks)], axis=1))
        q_t[at, :] = both[0:rank] + both[rank:]
    spots = [
        (slice(c // c_blocks * r_size, (c // c_blocks + 1) * r_size),
         slice(c % c_blocks * c_size, (c % c_blocks + 1) * c_size))
        for c in range(n)
    ]
    for c in range(n):
        q_part[c] = q_t[spots[c]].astype(BF16)
    q_rs[me] = q_part[me]
    for d in range(1, n):
        to = lax.rem(me + d, n)
        send(q_part.at[to], q_rs.at[me], to, grp, "term", "term")
    wait_all(q_rs.at[0:n - 1], "term", "term")
    total = q_rs[0].astype(F32)
    for k in range(1, n):
        total += q_rs[k].astype(F32)
    q_grp[grp] = total.astype(BF16)
    for d in range(1, g):
        send(q_grp.at[grp], q_grp.at[grp], me, lax.rem(grp + d, g), "group", "group")
    wait_all(q_grp.at[0:g - 1], "group", "group")
    total = q_grp[0].astype(F32)
    for k in range(1, g):
        total += q_grp[k].astype(F32)
    q_all[me] = (total * (1.0 / g)).astype(BF16)
    for d in range(1, n):
        send(q_all.at[me], q_all.at[me], lax.rem(me + d, n), grp, "right", "right")
    wait_all(q_all.at[0:n - 1], "right", "right")
    for c in range(n):
        q_t[spots[c]] = q_all[c].astype(F32)
    local(q_t.at[0:used], q_out, chunks + 7)

    lanes = lax.broadcasted_iota(jnp.int32, (rows, LANES), 1)
    right = q_t[...].astype(BF16)
    right = jnp.concatenate([right, right], axis=0)
    for m in range(3):
        own = jnp.where((lanes >= m * rank) & (lanes < (m + 1) * rank), hat, 0.0)
        top = own.astype(BF16)
        left = jnp.concatenate([top, (own - top.astype(F32)).astype(BF16)], axis=1)
        for c in range(chunks):
            at = slice(c * wide, (c + 1) * wide)
            rebuilt = dot(left, right[:, at])
            merged = jnp.concatenate([
                high[m, j, 0:rows].astype(F32) + low[m, j, 0:rows].astype(F32)
                for j in (2 * c, 2 * c + 1)
            ], axis=1)
            err_out[:, m * hidden + c * wide:m * hidden + (c + 1) * wide] = (
                merged - rebuilt
            ).astype(BF16)
        at = pl.ds(m * hidden, hidden)
        local(err_out.at[:, at], new_err.at[0, :, at], chunks + 5)
    others = n // 2 - 1
    leave_refs["plane"] = (full.at[0:chunks, :, 0:others * rows, :], leave_refs["plane"][1])
    leave_refs["twin"] = (leave_refs["plane"][0], leave_refs["twin"][1])
    leave_refs["pair"] = (full.at[0:chunks], leave_refs["pair"][1])
    for t in range(steps):
        leave_refs["reduce", t] = (recv_bufs[t], leave_refs["reduce", t][1])
    leave_refs["hidden"] = (their_hid, leave_refs["hidden"][1])
    leave_refs["back"] = (their_back, leave_refs["back"][1])
    for leave, (ref, arrive) in leave_refs.items():
        whole(ref, arrive, leave).wait_send()
    pltpu.make_async_copy(hat_out, p_out, local_sems.at[chunks + 6]).wait()
    pltpu.make_async_copy(q_t.at[0:used], q_out, local_sems.at[chunks + 7]).wait()
    pltpu.make_async_copy(tok_out, tok_grad, local_sems.at[chunks + 4]).wait()
    pltpu.make_async_copy(err_out, new_err.at[0], local_sems.at[chunks + 5]).wait()


def write_results(*refs):
    ins, outs, bufs, sems = refs[:4], refs[4:8], refs[8:12], refs[12]
    cuts = []
    for k in (0, 1, 2, 3):
        axis = len(ins[k].shape) - 2
        size = ins[k].shape[axis]
        count = 3 if k == 0 else 2 if k == 1 else 1
        for i in range(count):
            at = (slice(None),) * axis + (pl.ds(i * (size // count), size // count),)
            cuts.append((k, at))
    reads, writes = [], []
    for i, (k, at) in enumerate(cuts):
        reads.append(pltpu.make_async_copy(ins[k].at[at], bufs[k].at[at], sems.at[0, i]))
        reads[-1].start()
    for i, (k, at) in enumerate(cuts):
        reads[i].wait()
        writes.append(pltpu.make_async_copy(bufs[k].at[at], outs[k].at[at], sems.at[1, i]))
        writes[-1].start()
    for copy in writes:
        copy.wait()


def on_device(n, g, tokens, cotangent, gate_weight, up_weight, down_weight_t, error_memory, q_init):
    token_rows, depth = tokens.shape
    rows, hidden = gate_weight.shape
    rank = q_init.shape[2]
    used = 3 * rank
    bits = n.bit_length() - 1
    side = depth // 2
    wide = 2 * LANES
    chunks = hidden // wide
    blocks = hidden // LANES
    padded = -(-rows // LANES) * LANES
    q_rows = q_init.transpose(0, 2, 1).reshape(used, hidden)
    c_blocks = min(n, hidden // LANES)
    chunk = (used // (n // c_blocks), hidden // c_blocks)
    packed_rows = rows * 3 // 4 if rows % 32 == 0 and 4 * used == 3 * LANES else rows
    parts = 2 if rows % 32 == 0 else 1
    arrivals = (
        chunks * (bits - 1) * (parts + 1) + blocks + (2 * blocks + 1) * (bits - 1) + 2 * blocks + 6
    )
    leaves = 11 + bits - 1
    recv_shapes = [
        pltpu.VMEM((blocks * 3 + 1, 1 << (bits - 2 - t), rows, LANES), BF16) for t in range(bits - 1)
    ]
    hbm = pl.BlockSpec(memory_space=pl.ANY)
    token_grad, new_error, hat_t, q_t = pl.pallas_call(
        functools.partial(kernel, n, g, rank),
        out_shape=(
            jax.ShapeDtypeStruct((token_rows, depth), BF16),
            jax.ShapeDtypeStruct((1, rows, 3 * hidden), BF16),
            jax.ShapeDtypeStruct((used, rows), F32),
            jax.ShapeDtypeStruct((used, hidden), F32),
        ),
        in_specs=[hbm] * 7,
        out_specs=(hbm,) * 4,
        scratch_shapes=[
            pltpu.VMEM((2 * chunks, 3, depth, LANES), BF16),
            pltpu.VMEM((token_rows, depth), BF16),
            pltpu.VMEM((token_rows, depth), BF16),
            pltpu.VMEM((2, 2, side, token_rows), BF16),
            pltpu.VMEM((2, side, token_rows), BF16),
            pltpu.VMEM((token_rows, wide), F32),
            pltpu.VMEM((blocks, token_rows, LANES), BF16),
            pltpu.VMEM((blocks, token_rows, LANES), BF16),
            pltpu.VMEM((blocks, token_rows, wide), BF16),
            pltpu.VMEM((blocks, token_rows, wide), BF16),
            pltpu.VMEM((blocks + 1, 3, side, LANES), BF16),
            *recv_shapes,
            pltpu.VMEM((3, blocks, padded, LANES), BF16),
            pltpu.VMEM((3, blocks, padded, LANES), BF16),
            pltpu.VMEM((3, hidden, wide), BF16),
            pltpu.VMEM((rows, 3 * hidden), BF16),
            pltpu.VMEM((LANES, hidden), F32),
            pltpu.VMEM((token_rows, depth), BF16),
            pltpu.VMEM((rows, 3 * hidden), BF16),
            pltpu.VMEM((used, rows), F32),
            pltpu.VMEM((side, LANES), F32),
            pltpu.VMEM((rows, LANES), F32),
            pltpu.VMEM((padded, LANES), F32),
            pltpu.VMEM((LANES, LANES), F32),
            pltpu.VMEM((LANES, hidden), F32),
            pltpu.VMEM((g, packed_rows, LANES), BF16),
            pltpu.VMEM((n, rank, LANES), F32),
            pltpu.VMEM((n,) + chunk, BF16),
            pltpu.VMEM((n,) + chunk, BF16),
            pltpu.VMEM((g,) + chunk, BF16),
            pltpu.VMEM((n,) + chunk, BF16),
            pltpu.SemaphoreType.DMA((leaves,)),
            pltpu.SemaphoreType.DMA((arrivals,)),
            pltpu.SemaphoreType.DMA((chunks + 8,)),
        ],
        compiler_params=pltpu.CompilerParams(
            collective_id=0, has_side_effects=True, vmem_limit_bytes=67_043_328
        ),
    )(tokens, cotangent, gate_weight, up_weight, down_weight_t, error_memory, q_rows)
    results = (token_grad, new_error, hat_t, q_t)
    token_grad, new_error, hat_t, q_t = pl.pallas_call(
        write_results,
        out_shape=tuple(jax.ShapeDtypeStruct(r.shape, r.dtype) for r in results),
        in_specs=[hbm] * 4,
        out_specs=(hbm,) * 4,
        scratch_shapes=[
            *(pltpu.VMEM(r.shape, r.dtype) for r in results),
            pltpu.SemaphoreType.DMA((2, 8)),
        ],
    )(*results)
    p_hat = hat_t.reshape(3, rank, rows).transpose(0, 2, 1)
    q_new = q_t.reshape(3, rank, hidden).transpose(0, 2, 1)
    return token_grad, new_error, p_hat, q_new


def solution(mesh):
    return jax.shard_map(
        functools.partial(on_device, mesh.shape["node"], mesh.shape["grp"]),
        mesh=mesh,
        in_specs=(
            P(("node", "grp"), None),
            P(("node", "grp"), None),
            P("node", None),
            P("node", None),
            P("node", None),
            P("grp", "node", None),
            P(),
        ),
        out_specs=(P(("node", "grp"), None), P("grp", "node", None), P(None, "node", None), P()),
        check_vma=False,
    )
```

```python
import functools
import math

import jax
import jax.numpy as jnp
from jax import lax
from jax.experimental import pallas as pl
from jax.experimental.pallas import tpu as pltpu
from jax.sharding import PartitionSpec as P

MESH = pl.DeviceIdType.MESH
F32, BF16 = jnp.float32, jnp.bfloat16
HIGHEST = lax.Precision.HIGHEST
AHEAD, LAG, PIVOTS = 2, 4, 4
LANES = 128


def gelu_parts(value):
    coeff = math.sqrt(2.0 / math.pi)
    square = value * value
    tanh_value = jnp.tanh(coeff * (value + 0.044715 * square * value))
    activation = 0.5 * value * (1.0 + tanh_value)
    slope = 0.5 * (1.0 + tanh_value) + 0.5 * value * (1.0 - tanh_value * tanh_value) * coeff * (
        1.0 + 3.0 * 0.044715 * square
    )
    return activation, slope


def dot(a, b, precision=None):
    return jnp.dot(a, b, preferred_element_type=F32, precision=precision)


def dot_nt(a, b, precision=None):
    return lax.dot_general(
        a, b, (((1,), (1,)), ((), ())), preferred_element_type=F32, precision=precision
    )


def subsets(items):
    found = [()]
    for item in items:
        found += [s + (item,) for s in found]
    return found


def kernel(
    n, g, rank,
    tok_hbm, cot_hbm, w_gate, w_up, w_down, err_hbm, q_hbm,
    tok_grad, new_err, p_out, q_out,
    full, tok, cot, turned, turned_in, acts, mine_hid, their_hid, mine_back,
    their_back, grads, *rest
):
    bits = n.bit_length() - 1
    recv_bufs = rest[:bits - 1]
    (high, low, q_right, err, q_rows, tok_out, err_out, hat_out, early, pw_acc, power, block_diag, q_t, pw_all,
     gram_all, q_part, q_rs, q_grp, q_all, send_sems, recv_sems, local_sems) = rest[bits - 1:]
    me, grp = lax.axis_index("node"), lax.axis_index("grp")
    rows, hidden = w_gate.shape
    tokens, depth = tok.shape
    side = depth // 2
    wide = 2 * LANES
    chunks = hidden // wide
    blocks = hidden // LANES
    used = 3 * rank
    weights = (w_gate, w_up, w_down)

    barrier = pltpu.get_barrier_semaphore()
    for d in range(1, n):
        pl.semaphore_signal(barrier, inc=1, device_id=(lax.rem(me + d, n), grp), device_id_type=MESH)
    for d in range(1, g):
        pl.semaphore_signal(barrier, inc=1, device_id=(me, lax.rem(grp + d, g)), device_id_type=MESH)

    flip = [(1 << b) * (1 - 2 * lax.rem(me // (1 << b), 2)) for b in range(bits)]
    offset = lambda mask: sum((flip[b] for b in mask), 0)
    pair = me + flip[0]
    core = lax.rem(me, 2)
    half_node = me // 2
    half_flip = [0] + [
        (1 << (b - 1)) * (1 - 2 * lax.rem(me // (1 << b), 2)) for b in range(1, bits)
    ]
    half_offset = lambda mask: sum((half_flip[b] for b in mask), 0)
    plane = lax.rem(grp, 2)
    twin = grp + 1 - 2 * plane
    outer = list(range(1, bits))
    orders = [outer, outer[::-1]]
    steps = len(outer)
    block = lambda index: pl.ds(pl.multiple_of(index * rows, rows), rows)

    def local(src, dst, index):
        copy = pltpu.make_async_copy(src, dst, local_sems.at[index])
        copy.start()
        return copy

    for c in range(chunks):
        for j in (2 * c, 2 * c + 1):
            for w in range(3):
                local(weights[w].at[:, pl.ds(j * LANES, LANES)], full.at[j, w, block(me)], c)
    cot_load = local(cot_hbm, cot, chunks)
    tok_load = local(tok_hbm, tok, chunks + 1)
    q_load = local(q_hbm, q_rows.at[0:used], chunks + 2)
    err_load = local(err_hbm.at[0], err, chunks + 3)

    arrive_index, leave_index, leave_refs = {}, {}, {}

    def send(src, dst, node, group, arrive, leave):
        pltpu.make_async_remote_copy(
            src_ref=src, dst_ref=dst,
            send_sem=send_sems.at[leave_index.setdefault(leave, len(leave_index))],
            recv_sem=recv_sems.at[arrive_index.setdefault(arrive, len(arrive_index))],
            device_id=(node, group), device_id_type=MESH,
        ).start()

    def whole(ref, arrive, leave):
        return pltpu.make_async_remote_copy(
            src_ref=ref, dst_ref=ref,
            send_sem=send_sems.at[leave_index[leave]], recv_sem=recv_sems.at[arrive_index[arrive]],
            device_id=(me, twin), device_id_type=MESH,
        )

    def wait_all(ref, arrive, leave):
        leave_refs.setdefault(leave, (ref, arrive))
        whole(ref, arrive, leave).wait_recv()

    if rows % 32 == 0:
        row_parts = [[(0, rows // 2, 0), (rows // 2, rows // 2, 1)]] * chunks
    else:
        row_parts = [[(0, rows, c % 2)] for c in range(chunks)]
    parts = [
        [part + cut for cut in (((0, 1), (1, 1), (2, 1)) if c == 0 else ((0, 3),)) for part in row_parts[c]]
        for c in range(chunks)
    ]

    def piece(j, mask, part):
        start = (me + offset(mask)) * rows + part[0]
        at = pl.ds(pl.multiple_of(start, math.gcd(rows, part[1])), part[1])
        return full.at[j, pl.ds(part[3], part[4]), at, :]

    def column_block(side_of, c):
        return 2 * c + (plane if side_of == 0 else 1 - plane)

    def new_masks(t, order):
        return [mask + (order[t],) for mask in subsets(order[:t])]

    def gather_send(c, t, part):
        order = orders[part[2]]
        for mask in subsets(order[:t]):
            at = piece(2 * c + plane, mask, part)
            send(at, at, me + flip[order[t]], grp, ("plane", c, t, part), "plane")

    def gather_step(c, t):
        for part in parts[c]:
            wait_all(full.at[2 * c, pl.ds(0, part[4]), 0:part[1] << t, :], ("plane", c, t, part), "plane")
            if t + 1 < steps:
                gather_send(c, t + 1, part)
            for mask in new_masks(t, orders[part[2]]):
                at = piece(2 * c + plane, mask, part)
                send(at, at, me, twin, ("twin", c, t), "twin")
                send(at, at, pair, grp, ("pair", 0, c), "pair")

    def relay(c):
        for t in range(steps):
            wait_all(full.at[2 * c, :, 0:rows << t, :], ("twin", c, t), "twin")
            for part in parts[c]:
                for mask in new_masks(t, orders[part[2]]):
                    at = piece(2 * c + 1 - plane, mask, part)
                    send(at, at, pair, grp, ("pair", 1, c), "pair")

    pl.semaphore_wait(barrier, n - 1 + g - 1)

    def launch(c):
        at = full.at[pl.ds(2 * c, 2), :, block(me), :]
        pltpu.make_async_copy(at, at, local_sems.at[c]).wait()
        for part in parts[c]:
            gather_send(c, 0, part)
        for side_of in range(2):
            at = full.at[column_block(side_of, c), :, block(me), :]
            send(at, at, pair, grp, ("pair", side_of, c), "pair")

    for c in range(min(2, chunks)):
        launch(c)

    pw_acc[...] = jnp.zeros_like(pw_acc)
    early[...] = jnp.zeros_like(early)
    power[...] = jnp.zeros_like(power)
    block_diag[...] = jnp.zeros_like(block_diag)
    q_t[...] = jnp.zeros_like(q_t)
    for buf in (high, low):
        for m in range(3):
            for j in range(blocks):
                buf[m, j, rows:, :] = jnp.zeros((buf.shape[2] - rows, LANES), BF16)

    def turn(which, i):
        src = (tok, cot)[which]
        tile = src[:, i * wide:(i + 1) * wide].T
        first = i * wide
        while first < (i + 1) * wide:
            b = first // rows
            last = min((b + 1) * rows, (i + 1) * wide)
            at = (b // 2) * rows + first - b * rows
            turned[which, b % 2, at:at + last - first, :] = tile[first - i * wide:last - i * wide]
            first = last

    def right_factors():
        q_load.wait()
        q_rows[used:, :] = jnp.zeros((LANES - used, hidden), F32)
        lane = lax.broadcasted_iota(jnp.int32, (wide, LANES), 1)
        for c in range(chunks):
            at = slice(c * wide, (c + 1) * wide)
            columns = q_rows[:, at].T
            top = columns.astype(BF16)
            bottom = (columns - top.astype(F32)).astype(BF16)
            for m in range(3):
                inside_m = (lane >= m * rank) & (lane < (m + 1) * rank)
                q_right[m, at, 0:LANES] = jnp.where(inside_m, top.astype(F32), 0.0).astype(BF16)
                q_right[m, at, LANES:] = jnp.where(inside_m, bottom.astype(F32), 0.0).astype(BF16)

    units = [(0, c) for c in range(chunks)]
    for c in range(chunks):
        units.insert(min(chunks - 1 + 2 * c, len(units)), (1, c))
    extra = len(units)
    first_late = extra - (chunks - 1)

    def memory_power():
        err_load.wait()
        for side_of, c in units[first_late:]:
            j = column_block(side_of, c)
            at = pl.ds(pl.multiple_of(j * LANES, LANES), LANES)
            left = jnp.concatenate([
                err[:, pl.ds(pl.multiple_of(m * hidden + j * LANES, LANES), LANES)]
                for m in range(3)
            ], axis=1)
            both = dot(left, jnp.concatenate([q_right[m, at, :] for m in range(3)], axis=0))
            pw_acc[...] += both[:, 0:LANES] + both[:, LANES:]

    filler = []
    for which, load in ((1, cot_load), (0, tok_load)):
        filler.append(load.wait)
        for i in range(depth // wide):
            filler.append(functools.partial(turn, which, i))
        filler.append(functools.partial(
            send, turned.at[which, 1 - core], turned_in.at[which], pair, grp, "turned", "turned"))
    filler += [right_factors, memory_power]

    def forward(j):
        both = dot(tok[...], jnp.concatenate([full[j, 0], full[j, 1]], axis=1))
        acts[...] = both
        up_pre = acts[:, LANES:]
        activation, slope = gelu_parts(acts[:, 0:LANES])
        mine_hid[j] = (activation * up_pre).astype(BF16)
        acts[:, LANES:] = activation
        acts[:, 0:LANES] = up_pre * slope

    def backward(j):
        back = dot(cot[...], full[j, 2])
        mine_back[j, :, 0:LANES] = (back * acts[:, 0:LANES]).astype(BF16)
        mine_back[j, :, LANES:] = (back * acts[:, LANES:]).astype(BF16)

    tile = side // 2
    group_m = ((2,), (0, 1))

    def gradient(u, j, k):
        own, other = ((mine_hid, their_hid), (mine_back, their_back))[k]
        right = jnp.concatenate([own[j], other[j]], axis=0)
        for i in range(2):
            at = pl.ds(i * tile, tile)
            left = jnp.concatenate([turned[1 - k, core, at, :], turned_in[1 - k, at, :]], axis=1)
            part = dot(left, right).astype(BF16)
            for i, m in enumerate(group_m[k]):
                grads[u, m, at, :] = part[:, i * LANES:(i + 1) * LANES]

    slots_of = {2: 0, 0: 1, 1: 2}

    def reduce_start(u, k, t):
        for m in group_m[k]:
            for first, size, h in row_parts[u % chunks]:
                bit = orders[h][t]
                for slot, mask in enumerate(subsets(orders[h][t + 1:])):
                    at = half_node + half_flip[bit] + half_offset(mask)
                    at = pl.ds(pl.multiple_of(at * rows + first, math.gcd(rows, size)), size)
                    dst = recv_bufs[t].at[u * 3 + slots_of[m], slot, pl.ds(first, size)]
                    send(grads.at[u, m, at], dst, me + flip[bit], grp,
                         ("reduce", u, k, t), ("reduce", t))

    scale = 1.0 / math.sqrt(tokens * n)

    def reduce_add(u, j, k, t):
        wait_all(
            recv_bufs[t].at[pl.ds(u * 3 + k, 1 + k)], ("reduce", u, k, t), ("reduce", t))
        for m in group_m[k]:
            for first, size, h in row_parts[u % chunks]:
                for slot, mask in enumerate(subsets(orders[h][t + 1:])):
                    at = (half_node + half_offset(mask)) * rows + first
                    at = pl.ds(pl.multiple_of(at, math.gcd(rows, size)), size)
                    total = (
                        grads[u, m, at, :].astype(F32)
                        + recv_bufs[t][u * 3 + slots_of[m], slot, first:first + size].astype(F32)
                    )
                    if t < steps - 1:
                        grads[u, m, at, :] = total.astype(BF16)
                    elif u == extra:
                        pw_acc[first:first + size] += total * scale
                    else:
                        span = pl.ds(pl.multiple_of(m * hidden + j * LANES, LANES), LANES)
                        memory = err[first:first + size, span].astype(F32)
                        merged = total * scale + memory
                        top = merged.astype(BF16)
                        high[m, j, first:first + size] = top
                        low[m, j, first:first + size] = (merged - top.astype(F32)).astype(BF16)

    def reduce_finish(u, j, k):
        reduce_add(u, j, k, steps - 1)
        at = pl.ds(pl.multiple_of(j * LANES, LANES), LANES)
        for m in group_m[k] if u < first_late else ():
            both = dot(high[m, j, 0:rows], q_right[m, at, :])
            rest_part = dot(low[m, j, 0:rows], q_right[m, at, 0:LANES])
            pw_acc[...] += both[:, 0:LANES] + both[:, LANES:] + rest_part

    def token_part(i):
        at = slice(i * wide, (i + 1) * wide)
        total = jnp.zeros((tokens, wide), F32)
        for k in range(2):
            lanes_k = slice(k * LANES, (k + 1) * LANES)
            left = jnp.concatenate([mine_back[j, :, lanes_k] for j in range(blocks)], axis=1)
            right = jnp.concatenate([full[j, k, at, :] for j in range(blocks)], axis=1)
            total += dot_nt(left, right)
        tok_out[:, at] = total.astype(BF16)
        local(tok_out.at[:, at], tok_grad.at[:, at], chunks + 4)

    token_tiles = list(range(depth // wide))

    def token_work(amount):
        for _ in range(min(amount, len(token_tiles))):
            token_part(token_tiles.pop(0))


    def prepare(u):
        side_of, c = units[u]
        wait_all(full.at[2 * c, :, 0:side, :], ("pair", side_of, c), "pair")
        j = column_block(*units[u])
        forward(j)
        send(mine_hid.at[j], their_hid.at[j], pair, grp, ("hidden", u), "hidden")
        backward(j)
        send(mine_back.at[j], their_back.at[j], pair, grp, ("back", u), "back")

    def early_power(u, j):
        at = pl.ds(pl.multiple_of(j * LANES, LANES), LANES)
        right = jnp.concatenate([q_right[m, at, :] for m in range(3)], axis=0)
        for i in range(2):
            span = pl.ds(i * tile, tile)
            left = jnp.concatenate([grads[u, m, span, :] for m in range(3)], axis=1)
            both = dot(left, right)
            early[span, :] += both[:, 0:LANES] + both[:, LANES:]

    def reduce_all(u, sent, between):
        j = column_block(*units[u])
        wait_all(their_hid.at[j], ("hidden", u), "hidden")
        for k in range(2):
            if k == 1:
                between()
                wait_all(their_back.at[j], ("back", u), "back")
            gradient(u, j, k)
            if k in sent:
                reduce_start(u, k, 0)
        if u >= first_late:
            early_power(u, j)

    def advance(u, t):
        j = column_block(*units[u])
        for k in range(2):
            reduce_add(u, j, k, t - 1)
            reduce_start(u, k, t)

    def finish(u):
        j = column_block(*units[u])
        for k in range(2):
            reduce_finish(u, j, k)

    events = sorted(
        ((c, t) for c in range(chunks) for t in range(steps)), key=lambda e: (2 * e[1] + e[0], -e[1])
    )
    ready = [i for i, (_, t) in enumerate(events) if t == steps - 1]
    each = -(-len(filler) // (ready[0] + 1))
    last = len(units) - 1
    done_u, relayed = [0], [0]

    def front(sent=(0, 1), between=lambda: None):
        if done_u[0] == 0:
            wait_all(turned_in, "turned", "turned")
        reduce_all(done_u[0], sent, between)
        done_u[0] += 1

    for i, (c, t) in enumerate(events):
        for work in filler[:each]:
            work()
        filler = filler[each:]
        if i == len(events) - 1:
            relay(0)
            relayed[0] += 1
        gather_step(c, t)
        if t == 0 and c + 2 < chunks:
            launch(c + 2)
        if i > ready[0]:
            if t == steps - 1:
                front()
            if t < steps - 1 or c == chunks - 1:
                continue
        if t == steps - 1:
            prepare(done_u[0])
    behind = [0]

    def settle():
        u = behind[0]
        for t in range(1, steps):
            advance(u, t)
        if u >= LAG:
            finish(u - LAG)
        behind[0] += 1

    def relay_next(ahead):
        if ahead < last and units[ahead + 1][0] and relayed[0] < chunks:
            relay(relayed[0])
            relayed[0] += 1

    while done_u[0] <= last:
        ahead = done_u[0]
        prepare(ahead)
        front((0, 1) if ahead < last - 1 else (), functools.partial(relay_next, ahead))
        while ahead < last and behind[0] <= ahead - AHEAD:
            settle()
    grads[extra, 2] = early[...].astype(BF16)
    reduce_start(extra, 0, 0)
    reduce_start(last - 1, 0, 0)
    for u in range(max(behind[0] - LAG, 0), first_late):
        finish(u)
    for t in range(1, steps):
        reduce_add(extra, 0, 0, t - 1)
        reduce_start(extra, 0, t)
    reduce_start(last - 1, 1, 0)
    for u in range(behind[0], last - 1):
        for t in range(1, steps):
            advance(u, t)
    for k in range(2):
        reduce_start(last, k, 0)
    token_work(2)
    reduce_add(extra, 0, 0, steps - 1)

    packed = pw_all.shape[1] < rows
    if packed:
        head = pw_all.shape[1]
        spare = lax.broadcasted_iota(jnp.int32, (head, LANES), 1) >= used
        tail = pw_acc[head:, :]
        moved = jnp.concatenate(
            [pltpu.roll(tail, used - m * rank, 1) for m in range(3)], axis=0)
        pw_all[grp] = jnp.where(spare, moved, pw_acc[0:head, :]).astype(BF16)
    else:
        pw_all[grp] = pw_acc[...].astype(BF16)
    for d in range(1, g):
        send(pw_all.at[grp], pw_all.at[grp], me, lax.rem(grp + d, g), "power", "power")
    token_work(4)
    wait_all(pw_all.at[0:g - 1], "power", "power")
    total = pw_all[0].astype(F32)
    for k in range(1, g):
        total += pw_all[k].astype(F32)
    total = total * (1.0 / g)
    if packed:
        short = rows - head
        spot = lax.broadcasted_iota(jnp.int32, (short, LANES), 1) // rank
        tail = jnp.zeros((short, LANES), F32)
        for m in range(3):
            back = pltpu.roll(total[m * short:(m + 1) * short], LANES - used + m * rank, 1)
            tail = jnp.where(spot == m, back, tail)
        power[0:head, :] = jnp.where(spare, 0.0, total)
        power[head:rows, :] = tail
    else:
        power[0:rows, :] = total

    lane = lax.broadcasted_iota(jnp.int32, (rank, LANES), 1)
    row = lax.broadcasted_iota(jnp.int32, (rank, LANES), 0)
    padded = power[...]
    gram = dot(padded.T, padded, HIGHEST)
    picked = gram[0:rank]
    for m in range(1, 3):
        picked = jnp.where(lane >= m * rank, gram[m * rank:(m + 1) * rank], picked)
    gram_all[me] = picked
    for d in range(1, n):
        send(gram_all.at[me], gram_all.at[me], lax.rem(me + d, n), grp, "gram", "gram")
    for u in (last - 1, last):
        for t in range(1, steps):
            advance(u, t)
    for u in range(first_late, last - 1):
        finish(u)
    token_work(len(token_tiles))
    wait_all(gram_all.at[0:n - 1], "gram", "gram")
    picked = gram_all[0]
    for k in range(1, n):
        picked += gram_all[k]

    work = []
    for m in range(3):
        rolled = picked if m == 0 else pltpu.roll(picked, LANES - m * rank, 1)
        unit = jnp.where(lane == row + rank, 1.0, 0.0).astype(F32)
        work.append(jnp.where(lane < rank, rolled, unit))
    for first in range(0, rank, PIVOTS):
        for m in range(3):
            a = work[m]
            pivots = range(PIVOTS)
            spread = [
                jnp.broadcast_to(a[:, first + i:first + i + 1], (rank, LANES)) for i in pivots
            ]
            pivot_rows = [a[first + i:first + i + 1, :] for i in pivots]
            update = None
            for i in pivots:
                inverse = 1.0 / spread[i][first + i:first + i + 1, :]
                for k in range(i + 1, PIVOTS):
                    factor = spread[i][first + k:first + k + 1, :] * inverse
                    spread[k] -= spread[i] * factor
                    pivot_rows[k] -= pivot_rows[i] * factor
                term = spread[i] * (pivot_rows[i] * inverse)
                update = term if update is None else update + term
            a = jnp.where(row >= first + PIVOTS, a - update, a)
            for i in pivots:
                a = jnp.where(row == first + i, pivot_rows[i], a)
            work[m] = a
    for m in range(3):
        diagonal = jnp.sum(jnp.where(lane == row, work[m], 0.0), axis=1, keepdims=True)
        work[m] = work[m] * (1.0 / jnp.sqrt(diagonal))
    for m in range(3):
        shift = ((m - 1) * rank) % LANES
        moved = work[m] if shift == 0 else pltpu.roll(work[m], shift, 1)
        inside_m = (lane >= m * rank) & (lane < (m + 1) * rank)
        block_diag[m * rank:(m + 1) * rank, :] = jnp.where(inside_m, moved, 0.0)
    hat_t = dot_nt(block_diag[...], power[...], HIGHEST)
    hat = dot_nt(power[0:rows, :], block_diag[...], HIGHEST)
    hat_out[...] = hat_t[0:used, 0:rows]
    local(hat_out, p_out, chunks + 6)

    c_blocks = min(n, hidden // LANES)
    r_blocks = n // c_blocks
    c_size, r_size = hidden // c_blocks, used // r_blocks
    hat_top = hat_t.astype(BF16)
    hat_bottom = (hat_t - hat_top.astype(F32)).astype(BF16)
    spots = [
        (slice(c // c_blocks * r_size, (c // c_blocks + 1) * r_size),
         slice(c % c_blocks * c_size, (c % c_blocks + 1) * c_size))
        for c in range(n)
    ]

    def right_terms(first, end):
        for m in range(3):
            at = slice(m * rank, (m + 1) * rank)
            left = jnp.concatenate([hat_top[at], hat_bottom[at]], axis=0)
            both = dot(left, jnp.concatenate([high[m, j] for j in range(first, end)], axis=1))
            q_t[at, first * LANES:end * LANES] = both[0:rank] + both[rank:]
        for c in range(n):
            if first * LANES <= spots[c][1].start and spots[c][1].stop <= end * LANES:
                q_part[c] = q_t[spots[c]].astype(BF16)

                @pl.when(me != c)
                def _():
                    send(q_part.at[c], q_rs.at[me], c, grp, "term", "term")

    finish(last - 1)
    right_terms(0, blocks - 2)
    finish(last)
    right_terms(blocks - 2, blocks)
    q_rs[me] = q_part[me]
    wait_all(q_rs.at[0:n - 1], "term", "term")
    total = q_rs[0].astype(F32)
    for k in range(1, n):
        total += q_rs[k].astype(F32)
    q_grp[grp] = total.astype(BF16)
    for d in range(1, g):
        send(q_grp.at[grp], q_grp.at[grp], me, lax.rem(grp + d, g), "group", "group")
    wait_all(q_grp.at[0:g - 1], "group", "group")
    total = q_grp[0].astype(F32)
    for k in range(1, g):
        total += q_grp[k].astype(F32)
    q_all[me] = (total * (1.0 / g)).astype(BF16)
    for d in range(1, n):
        send(q_all.at[me], q_all.at[me], lax.rem(me + d, n), grp, "right", "right")
    wait_all(q_all.at[0:n - 1], "right", "right")
    for c in range(n):
        q_t[spots[c]] = q_all[c].astype(F32)
    local(q_t.at[0:used], q_out, chunks + 7)

    lanes = lax.broadcasted_iota(jnp.int32, (rows, LANES), 1)
    right = q_t[...].astype(BF16)
    right = jnp.concatenate([right, right], axis=0)
    for m in range(3):
        own = jnp.where((lanes >= m * rank) & (lanes < (m + 1) * rank), hat, 0.0)
        top = own.astype(BF16)
        left = jnp.concatenate([top, (own - top.astype(F32)).astype(BF16)], axis=1)
        for c in range(chunks):
            at = slice(c * wide, (c + 1) * wide)
            rebuilt = dot(left, right[:, at])
            merged = jnp.concatenate([
                high[m, j, 0:rows].astype(F32) + low[m, j, 0:rows].astype(F32)
                for j in (2 * c, 2 * c + 1)
            ], axis=1)
            err_out[:, m * hidden + c * wide:m * hidden + (c + 1) * wide] = (
                merged - rebuilt
            ).astype(BF16)
        at = pl.ds(m * hidden, hidden)
        local(err_out.at[:, at], new_err.at[0, :, at], chunks + 5)
    others = n // 2 - 1
    leave_refs["plane"] = (full.at[0:chunks, :, 0:others * rows, :], leave_refs["plane"][1])
    leave_refs["twin"] = (leave_refs["plane"][0], leave_refs["twin"][1])
    leave_refs["pair"] = (full.at[0:chunks], leave_refs["pair"][1])
    for t in range(steps):
        leave_refs["reduce", t] = (recv_bufs[t], leave_refs["reduce", t][1])
    leave_refs["hidden"] = (their_hid, leave_refs["hidden"][1])
    leave_refs["back"] = (their_back, leave_refs["back"][1])
    for leave, (ref, arrive) in leave_refs.items():
        whole(ref, arrive, leave).wait_send()
    pltpu.make_async_copy(hat_out, p_out, local_sems.at[chunks + 6]).wait()
    pltpu.make_async_copy(q_t.at[0:used], q_out, local_sems.at[chunks + 7]).wait()
    pltpu.make_async_copy(tok_out, tok_grad, local_sems.at[chunks + 4]).wait()
    pltpu.make_async_copy(err_out, new_err.at[0], local_sems.at[chunks + 5]).wait()


def write_results(*refs):
    ins, outs, bufs, sems = refs[:4], refs[4:8], refs[8:12], refs[12]
    cuts = []
    for k in (0, 1, 2, 3):
        axis = len(ins[k].shape) - 2
        size = ins[k].shape[axis]
        count = 3 if k == 0 else 2 if k == 1 else 1
        for i in range(count):
            at = (slice(None),) * axis + (pl.ds(i * (size // count), size // count),)
            cuts.append((k, at))
    reads, writes = [], []
    for i, (k, at) in enumerate(cuts):
        reads.append(pltpu.make_async_copy(ins[k].at[at], bufs[k].at[at], sems.at[0, i]))
        reads[-1].start()
    for i, (k, at) in enumerate(cuts):
        reads[i].wait()
        writes.append(pltpu.make_async_copy(bufs[k].at[at], outs[k].at[at], sems.at[1, i]))
        writes[-1].start()
    for copy in writes:
        copy.wait()


def on_device(n, g, tokens, cotangent, gate_weight, up_weight, down_weight_t, error_memory, q_init):
    token_rows, depth = tokens.shape
    rows, hidden = gate_weight.shape
    rank = q_init.shape[2]
    used = 3 * rank
    bits = n.bit_length() - 1
    side = depth // 2
    wide = 2 * LANES
    chunks = hidden // wide
    blocks = hidden // LANES
    padded = -(-rows // LANES) * LANES
    q_rows = q_init.transpose(0, 2, 1).reshape(used, hidden)
    c_blocks = min(n, hidden // LANES)
    chunk = (used // (n // c_blocks), hidden // c_blocks)
    packed_rows = rows * 3 // 4 if rows % 32 == 0 and 4 * used == 3 * LANES else rows
    parts = 2 if rows % 32 == 0 else 1
    arrivals = (
        (bits - 1) * (chunks * (parts + 1) + 2 * parts) + blocks + (2 * blocks + 1) * (bits - 1) + 2 * blocks + 6
    )
    leaves = 11 + bits - 1
    recv_shapes = [
        pltpu.VMEM((blocks * 3 + 1, 1 << (bits - 2 - t), rows, LANES), BF16) for t in range(bits - 1)
    ]
    hbm = pl.BlockSpec(memory_space=pl.ANY)
    token_grad, new_error, hat_t, q_t = pl.pallas_call(
        functools.partial(kernel, n, g, rank),
        out_shape=(
            jax.ShapeDtypeStruct((token_rows, depth), BF16),
            jax.ShapeDtypeStruct((1, rows, 3 * hidden), BF16),
            jax.ShapeDtypeStruct((used, rows), F32),
            jax.ShapeDtypeStruct((used, hidden), F32),
        ),
        in_specs=[hbm] * 7,
        out_specs=(hbm,) * 4,
        scratch_shapes=[
            pltpu.VMEM((2 * chunks, 3, depth, LANES), BF16),
            pltpu.VMEM((token_rows, depth), BF16),
            pltpu.VMEM((token_rows, depth), BF16),
            pltpu.VMEM((2, 2, side, token_rows), BF16),
            pltpu.VMEM((2, side, token_rows), BF16),
            pltpu.VMEM((token_rows, wide), F32),
            pltpu.VMEM((blocks, token_rows, LANES), BF16),
            pltpu.VMEM((blocks, token_rows, LANES), BF16),
            pltpu.VMEM((blocks, token_rows, wide), BF16),
            pltpu.VMEM((blocks, token_rows, wide), BF16),
            pltpu.VMEM((blocks + 1, 3, side, LANES), BF16),
            *recv_shapes,
            pltpu.VMEM((3, blocks, padded, LANES), BF16),
            pltpu.VMEM((3, blocks, padded, LANES), BF16),
            pltpu.VMEM((3, hidden, wide), BF16),
            pltpu.VMEM((rows, 3 * hidden), BF16),
            pltpu.VMEM((LANES, hidden), F32),
            pltpu.VMEM((token_rows, depth), BF16),
            pltpu.VMEM((rows, 3 * hidden), BF16),
            pltpu.VMEM((used, rows), F32),
            pltpu.VMEM((side, LANES), F32),
            pltpu.VMEM((rows, LANES), F32),
            pltpu.VMEM((padded, LANES), F32),
            pltpu.VMEM((LANES, LANES), F32),
            pltpu.VMEM((LANES, hidden), F32),
            pltpu.VMEM((g, packed_rows, LANES), BF16),
            pltpu.VMEM((n, rank, LANES), F32),
            pltpu.VMEM((n,) + chunk, BF16),
            pltpu.VMEM((n,) + chunk, BF16),
            pltpu.VMEM((g,) + chunk, BF16),
            pltpu.VMEM((n,) + chunk, BF16),
            pltpu.SemaphoreType.DMA((leaves,)),
            pltpu.SemaphoreType.DMA((arrivals,)),
            pltpu.SemaphoreType.DMA((chunks + 8,)),
        ],
        compiler_params=pltpu.CompilerParams(
            collective_id=0, has_side_effects=True, vmem_limit_bytes=67_043_328
        ),
    )(tokens, cotangent, gate_weight, up_weight, down_weight_t, error_memory, q_rows)
    results = (token_grad, new_error, hat_t, q_t)
    token_grad, new_error, hat_t, q_t = pl.pallas_call(
        write_results,
        out_shape=tuple(jax.ShapeDtypeStruct(r.shape, r.dtype) for r in results),
        in_specs=[hbm] * 4,
        out_specs=(hbm,) * 4,
        scratch_shapes=[
            *(pltpu.VMEM(r.shape, r.dtype) for r in results),
            pltpu.SemaphoreType.DMA((2, 8)),
        ],
    )(*results)
    p_hat = hat_t.reshape(3, rank, rows).transpose(0, 2, 1)
    q_new = q_t.reshape(3, rank, hidden).transpose(0, 2, 1)
    return token_grad, new_error, p_hat, q_new


def solution(mesh):
    return jax.shard_map(
        functools.partial(on_device, mesh.shape["node"], mesh.shape["grp"]),
        mesh=mesh,
        in_specs=(
            P(("node", "grp"), None),
            P(("node", "grp"), None),
            P("node", None),
            P("node", None),
            P("node", None),
            P("grp", "node", None),
            P(),
        ),
        out_specs=(P(("node", "grp"), None), P("grp", "node", None), P(None, "node", None), P()),
        check_vma=False,
    )
```
